256 devices in a mesh: seq: 32 (over y, z), mp: 8 (over x, core).
Axes of the slice: x: 4, y: 4, z: 8, core: 2. Of those that a mesh axis runs over, the one named last changes fastest.
Arguments:
- tokens: bfloat16 [12288, 2048], P('seq'), may hold values from -24 to 24
- database: bfloat16 [256, 96, 896], P('seq'), may hold values from -24 to 24
- nb_shard: int32 [192, 2], replicated, may hold values from 0 to 31, all different within a row; in each aligned block of 6 rows (0 to 5, 6 to 11, ...) no two rows name the same one
- nb_row: int32 [192, 2], replicated, may hold values from 0 to 7
- dec_gain: float32 [2048], replicated, may hold values from 0.1 to 1.9
- enc_gain: float32 [896], replicated, may hold values from 0.1 to 1.9
- w_in: bfloat16 [896, 1792], replicated, may hold values from -0.1875 to 0.1875
- w_out: bfloat16 [1792, 896], replicated, may hold values from -0.125 to 0.125
- w_query: bfloat16 [2048, 2048], P(None, 'mp'), may hold values from -0.125 to 0.125
- w_key: bfloat16 [896, 2048], P(None, 'mp'), may hold values from -0.1875 to 0.1875
- w_value: bfloat16 [896, 2048], P(None, 'mp'), may hold values from -0.1875 to 0.1875
- w_proj: bfloat16 [2048, 2048], P('mp'), may hold values from -0.5 to 0.5
- grad_out: bfloat16 [12288, 2048], P('seq'), may hold values from -6 to 6
Outputs:
- cca: bfloat16 [12288, 2048], P('seq', 'mp')
- grad_tokens: float32 [12288, 2048], P('seq', 'mp')
- grad_database: float32 [256, 96, 896], P('seq', 'mp')
The draws below stay inside these ranges and needn't reach their ends.
Inputs may be any that keep to these rules, and one draw needn't show every extreme that they name: `nb_shard`: in each aligned block of 6 stretches (the stretches of one device) no shard is named more than 1 times, and some block reaches it; the 2 neighbours of a stretch come from different shards.
All inputs are finite; a program needn't handle non-finite values.
Results may differ from the reference program's by a relative error of at most 0.017.
Values may be sent and summed in bfloat16 or wider, within the bound.
A program may use at most 128 MiB of HBM per device.

```python
import math
import jax
import jax.numpy as jnp
import numpy as np
from jax import lax

D = 2048
HEADS = 16
HD = 128
E = 896
F = 1792
L = 96
STRETCH = 64
K = 2
SEQ_LEN = 4096
ROWS_DEV = 8
CH_DEV = 6
CAP = 1
TOKENS = 12288
STRETCHES = 192
DBROWS = 256
N_SEQ = 32


def scale_field(key, base, row_shape, col_shape):
    key_row, key_col = jax.random.split(jax.random.fold_in(key, 17))
    col_scale = jnp.exp(jax.random.uniform(key_col, col_shape, minval=math.log(0.2), maxval=math.log(2.0)))
    row_scale = jnp.exp(jax.random.uniform(key_row, row_shape, minval=math.log(0.3), maxval=math.log(3.0)))
    return (base * col_scale * row_scale).astype(jnp.bfloat16)


def draw_tokens(key, part):
    key_base = jax.random.fold_in(key, 0)
    base = jnp.clip(jax.random.normal(key_base, (TOKENS, D)), -4.0, 4.0)
    return scale_field(key, base, (TOKENS, 1), (1, D))


def draw_database(key, part):
    key_base = jax.random.fold_in(key, 0)
    base = jnp.clip(jax.random.normal(key_base, (DBROWS, L, E)), -4.0, 4.0)
    return scale_field(key, base, (DBROWS, L, 1), (1, 1, E))


def with_ends(result, key, least, largest):
    spot = [jax.random.randint(jax.random.fold_in(key, axis), (), 0, length) for axis, length in enumerate(result.shape)]
    widest = result.shape.index(max(result.shape))
    next_to = spot[:widest] + [(spot[widest] + 1) % result.shape[widest]] + spot[widest + 1:]
    return result.at[tuple(spot)].set(least).at[tuple(next_to)].set(largest)


def levels(stream_key, extent, cuts, low, top_value):
    level = 1.0
    for position, parts in cuts:
        steps = jax.random.uniform(jax.random.fold_in(jax.random.fold_in(stream_key, 6), position), (parts,), jnp.float32, low / len(cuts), top_value / len(cuts))
        level = level * jnp.repeat(jnp.exp(steps), extent[position] // parts).reshape((-1,) + (1,) * (len(extent) - 1 - position))
    return level


def assign_block(own_key, own, number, rows, amount, top, most, skew):
    ranking = jax.random.permutation(own_key, amount)
    packed, usual = load_shares(amount, rows * top, most, skew, True), load_shares(amount, rows * top, most, skew, False)
    places = jnp.arange(amount)

    def named(tallies, turn):
        used = int((tallies > 0).sum())
        fixed = max(1, used // 4)
        passed = fixed + (places - fixed + turn * (used - fixed)) % max(1, amount - fixed)
        return jnp.zeros((amount,), jnp.int32).at[ranking[jnp.where(places < fixed, places, passed)]].set(jnp.asarray(tallies, jnp.int32))

    tallies = jnp.where(number % 4 == 0, named(packed, number // 4), named(usual, number - number // 4 - 1))
    mixed = jax.random.permutation(jax.random.fold_in(own, 3), amount)
    source_of, receiver = mixed[0:amount // 2 * 2:2], mixed[1:amount // 2 * 2:2]
    margin = jnp.minimum(tallies[source_of] - 1, most - tallies[receiver]) // 2
    margin = jnp.where((source_of == ranking[0]) | (receiver == ranking[0]) | (tallies[receiver] == 0), 0, jnp.maximum(margin, 0))
    passed = jax.random.randint(jax.random.fold_in(own, 4), (amount // 2,), 0, 1 << 20) % (margin + 1)
    tallies = tallies.at[source_of].add(-passed).at[receiver].add(passed)
    items = jnp.searchsorted(jnp.cumsum(tallies), jnp.arange(rows * top), side="right").astype(jnp.int32)
    listing = items.reshape(top, rows).T
    listing = listing[jax.random.permutation(jax.random.fold_in(own, 1), rows)]
    turn = jax.random.randint(jax.random.fold_in(own, 2), (rows, 1), 0, top)
    return jnp.take_along_axis(listing, (jnp.arange(top)[None, :] + turn) % top, axis=1)


def load_shares(number_of, total, bound, lean, full):
    portions = [(1 << 20) // math.isqrt(rank ** lean) + 1 for rank in range(1, number_of + 1)]
    largest = bound if full else min(bound, max(-(-total // number_of), total * portions[0] // sum(portions)))
    least = 1 if total - largest >= number_of - 1 else 0
    given, spare = [largest] + [least] * (number_of - 1), total - largest - least * (number_of - 1)
    while spare > 0:
        free = [i for i in range(1, number_of) if given[i] < largest] or [i for i in range(1, number_of) if given[i] < bound]
        pool, remaining = sum([portions[i] for i in free]), spare
        for i in free:
            extra = min(bound - given[i], max(1, remaining * portions[i] // pool), spare)
            given[i] = given[i] + extra
            spare = spare - extra
    return np.array(given)


def scatter_about(stream_key, shape, deviation, limit, cuts=(), dtype=jnp.bfloat16):
    loudness = levels(stream_key, shape, cuts, -0.22, 0.18) if cuts else 1.0
    entries = jax.random.normal(stream_key, shape, jnp.float32) * deviation * loudness
    return jnp.minimum(jnp.maximum(entries, -limit), limit).astype(dtype)


def setup_inputs(seed: int = 0) -> dict:
    arg_keys = jax.random.split(jax.random.key(seed), 14)
    tokens = draw_tokens(jax.random.fold_in(arg_keys[13], 71), 0)
    database = draw_database(jax.random.fold_in(arg_keys[13], 71), 0)
    nb_shard_keys = jax.random.split(jax.random.fold_in(arg_keys[2], 1), STRETCHES // CH_DEV)
    nb_shard_turns = jax.random.permutation(jax.random.fold_in(arg_keys[2], 3), STRETCHES // CH_DEV)
    nb_shard = jax.vmap(lambda own, number: assign_block(jax.random.fold_in(arg_keys[2], 2), own, number, CH_DEV, N_SEQ, K, CAP, 2))(nb_shard_keys, nb_shard_turns).reshape((STRETCHES, K))
    nb_row = with_ends(jax.random.randint(arg_keys[3], (STRETCHES, K), 0, ROWS_DEV), jax.random.fold_in(arg_keys[3], 1), 0, ROWS_DEV - 1).astype(jnp.int32)
    dec_gain = jnp.clip(1.0 + 0.18 * jax.random.normal(arg_keys[4], (D,), jnp.float32), 0.1, 1.9)
    enc_gain = jnp.clip(1.0 + 0.18 * jax.random.normal(arg_keys[5], (E,), jnp.float32), 0.1, 1.9)
    w_in = scatter_about(arg_keys[6], (E, F), E ** -0.5, 0.1875)
    w_out = scatter_about(arg_keys[7], (F, E), F ** -0.5, 0.125)
    w_query = scatter_about(arg_keys[8], (D, D), D ** -0.5, 0.125, ((1, 8),))
    w_key = scatter_about(arg_keys[9], (E, D), E ** -0.5, 0.1875, ((1, 8),))
    w_value = scatter_about(arg_keys[10], (E, D), E ** -0.5, 0.1875, ((1, 8),))
    w_proj = scatter_about(arg_keys[11], (D, D), HD ** -0.5, 0.5, ((0, 8),))
    grad_out = scatter_about(arg_keys[12], (TOKENS, D), 1.0, 6.0, ((0, 32),))
    return {"tokens": tokens, "database": database, "nb_shard": nb_shard, "nb_row": nb_row, "dec_gain": dec_gain, "enc_gain": enc_gain, "w_in": w_in, "w_out": w_out, "w_query": w_query, "w_key": w_key, "w_value": w_value, "w_proj": w_proj, "grad_out": grad_out}


EPSILON = 1e-06

def rms_scaling(values):
    return lax.rsqrt(lax.optimization_barrier(jnp.mean(values * values, axis=-1, keepdims=True)) + EPSILON)

def silu_slope(pre_act):
    sigmoid = jax.nn.sigmoid(pre_act)
    return sigmoid * (1.0 + pre_act * (1.0 - sigmoid))

def dot_t(matrix, weight):
    return lax.dot_general(matrix, weight, (((1,), (1,)), ((), ())), preferred_element_type=jnp.float32)

def reference(tokens, database, nb_shard, nb_row, dec_gain, enc_gain, w_in, w_out, w_query, w_key, w_value, w_proj, grad_out):
    flat_rows = (nb_shard * ROWS_DEV + nb_row).reshape(-1).astype(jnp.int32)
    embedded = jnp.take(database, flat_rows, axis=0).reshape(-1, E)
    values = embedded.astype(jnp.float32)
    scaling = rms_scaling(values)
    unit_rows = values * scaling
    enc_scale = enc_gain.astype(jnp.float32)
    normed = (unit_rows * enc_scale).astype(jnp.bfloat16)
    pre_act = jnp.dot(normed, w_in, preferred_element_type=jnp.float32)
    hidden = jax.nn.silu(pre_act).astype(jnp.bfloat16)
    encoded = (values + jnp.dot(hidden, w_out, preferred_element_type=jnp.float32)).astype(jnp.bfloat16)
    key_rows = jnp.dot(encoded, w_key, preferred_element_type=jnp.float32).astype(jnp.bfloat16)
    value_rows = jnp.dot(encoded, w_value, preferred_element_type=jnp.float32).astype(jnp.bfloat16)
    tok_vals = tokens.astype(jnp.float32)
    tok_scaling = rms_scaling(tok_vals)
    tok_unit = tok_vals * tok_scaling
    dec_scale = dec_gain.astype(jnp.float32)
    tok_normed = (tok_unit * dec_scale).astype(jnp.bfloat16)
    query_rows = jnp.dot(tok_normed, w_query, preferred_element_type=jnp.float32).astype(jnp.bfloat16)
    query_blk = query_rows.reshape(STRETCHES, STRETCH, HEADS, HD).astype(jnp.float32)
    key_blk = key_rows.reshape(STRETCHES, K * L, HEADS, HD).astype(jnp.float32)
    value_blk = value_rows.reshape(STRETCHES, K * L, HEADS, HD).astype(jnp.float32)
    factor = HD ** (-0.5)
    scores = jnp.einsum('cqhd,ckhd->chqk', query_blk, key_blk) * factor
    exp_score = jnp.exp(scores)
    attn_prob = exp_score / lax.optimization_barrier(jnp.sum(exp_score, axis=-1, keepdims=True))
    attn_weight = attn_prob.astype(jnp.bfloat16).astype(jnp.float32)
    context = jnp.einsum('chqk,ckhd->cqhd', attn_weight, value_blk).astype(jnp.bfloat16).reshape(TOKENS, D)
    live_tok = (jnp.arange(TOKENS) // STRETCH % (SEQ_LEN // STRETCH) != 0)[:, None]
    cca = jnp.where(live_tok, jnp.dot(context, w_proj, preferred_element_type=jnp.float32), 0.0).astype(jnp.bfloat16)
    masked = jnp.where(live_tok, grad_out, jnp.zeros_like(grad_out))
    grad_ctx = dot_t(masked, w_proj).astype(jnp.bfloat16)
    grad_blk = grad_ctx.reshape(STRETCHES, STRETCH, HEADS, HD).astype(jnp.float32)
    grad_prob = jnp.einsum('cqhd,ckhd->chqk', grad_blk, value_blk)
    grad_score = (attn_prob * (grad_prob - lax.optimization_barrier(jnp.sum(attn_prob * grad_prob, axis=-1, keepdims=True))) * factor).astype(jnp.bfloat16).astype(jnp.float32)
    grad_value = jnp.einsum('chqk,cqhd->ckhd', attn_weight, grad_blk).astype(jnp.bfloat16).reshape(-1, D)
    grad_query = jnp.einsum('chqk,ckhd->cqhd', grad_score, key_blk).astype(jnp.bfloat16).reshape(TOKENS, D)
    grad_key = jnp.einsum('chqk,cqhd->ckhd', grad_score, query_blk).astype(jnp.bfloat16).reshape(-1, D)
    grad_normed = dot_t(grad_query, w_query)
    tok_grad = grad_normed * dec_scale
    grad_tokens = tok_scaling * (tok_grad - tok_unit * lax.optimization_barrier(jnp.mean(tok_grad * tok_unit, axis=-1, keepdims=True)))
    grad_enc = dot_t(grad_key, w_key) + dot_t(grad_value, w_value)
    grad_hidden = dot_t(grad_enc.astype(jnp.bfloat16), w_out)
    grad_pre = (grad_hidden * silu_slope(pre_act)).astype(jnp.bfloat16)
    grad_unit = dot_t(grad_pre, w_in) * enc_scale
    grad_embed = grad_enc + scaling * (grad_unit - unit_rows * lax.optimization_barrier(jnp.mean(grad_unit * unit_rows, axis=-1, keepdims=True)))
    grad_database = jnp.zeros((DBROWS, L, E), jnp.float32).at[flat_rows].add(grad_embed.reshape(-1, L, E))
    return (cca, grad_tokens, grad_database)
```

```python
import functools

import jax
import jax.numpy as jnp
from jax import lax
from jax.experimental import pallas as pl
from jax.experimental.pallas import tpu as pltpu
from jax.sharding import Mesh
from jax.sharding import PartitionSpec as P

HD = 128
STRETCH = 64
K = 2
SEQ_LEN = 4096
UNIT = 8
EPSILON = 1e-06
MP = ("mp_0", "mp_1")
F32 = jnp.float32
BF16 = jnp.bfloat16
VM = pl.BlockSpec(memory_space=pltpu.VMEM)
SM = pl.BlockSpec(memory_space=pltpu.SMEM)
HB = pl.BlockSpec(memory_space=pltpu.HBM)
BIG = 64000 * 1024


def rcopy(src, dst, ssem, rsem, **where):
    return pltpu.make_async_remote_copy(
        src_ref=src,
        dst_ref=dst,
        send_sem=ssem,
        recv_sem=rsem,
        device_id=where,
        device_id_type=pl.DeviceIdType.MESH,
    )


def dot(a, b, ca=1, cb=0):
    return lax.dot_general(a, b, (((ca,), (cb,)), ((), ())), preferred_element_type=F32)


def rms_scaling(values):
    return lax.rsqrt(jnp.mean(values * values, axis=-1, keepdims=True) + EPSILON)


def sigmoid(v):
    return 1.0 / (1.0 + jnp.exp(-v))


def greet(n_seq, nx):
    me, x, c = lax.axis_index("seq"), lax.axis_index("mp_0"), lax.axis_index("mp_1")
    barrier = pltpu.get_barrier_semaphore()

    def tell(**where):
        pl.semaphore_signal(barrier, inc=1, device_id=where, device_id_type=pl.DeviceIdType.MESH)

    def far(k, carry):
        tell(seq=lax.rem(me + k, n_seq))
        return carry

    lax.fori_loop(1, n_seq, far, 0)
    tell(mp_0=lax.rem(x + 1, nx))
    tell(mp_0=lax.rem(x + nx - 1, nx))
    tell(mp_1=1 - c)
    return barrier, n_seq + 2


def seq_exchange(n_seq, n, src, dst, send, recv):
    me = lax.axis_index("seq")

    def piece(k, sending):
        peer = lax.rem(me + k, n_seq) if sending else lax.rem(me + n_seq - k, n_seq)
        at = me if sending else peer
        return rcopy(
            src.at[peer, pl.ds(0, n)],
            dst.at[at, pl.ds(0, n)],
            send.at[peer],
            recv.at[at],
            seq=peer,
        )

    def start():
        def go(k, carry):
            piece(k, True).start()
            return carry

        lax.fori_loop(1, n_seq, go, 0)

    def arrive():
        def go(k, carry):
            piece(k, False).wait_recv()
            return carry

        lax.fori_loop(1, n_seq, go, 0)

    def drain():
        def go(k, carry):
            piece(k, True).wait_send()
            return carry

        lax.fori_loop(1, n_seq, go, 0)

    return start, arrive, drain


def fetch_kernel(
    dims,
    codes, db, egain, w_in, w_out, tok, gout, dgain, w_q, w_p,
    full, q, gctx,
    win_v, w_in_v, w_out_v, tok_v, gout_v, w_q_v, w_p_v, enc, outg, recv, rows_s,
    lsem, a_send, a_recv, b_send, b_recv,
):
    n_seq, nx, nb, rows_dev, e = dims
    me, x, c = lax.axis_index("seq"), lax.axis_index("mp_0"), lax.axis_index("mp_1")
    barrier, greeted = greet(n_seq, nx)
    loads = [
        pltpu.make_async_copy(s, d, lsem.at[i])
        for i, (s, d) in enumerate(
            (
                (db.at[:, pl.ds(3 * x + c, 2)], win_v),
                (w_in, w_in_v),
                (w_out, w_out_v),
                (tok, tok_v),
                (w_q, w_q_v),
                (gout, gout_v),
                (w_p, w_p_v),
            )
        )
    ]
    for load in loads:
        load.start()

    def find(d, carry):
        row = jnp.int32(0)
        for k in range(nb):
            code = codes[d * nb + k]
            row = jnp.where(code // rows_dev == me, lax.rem(code, rows_dev), row)
        rows_s[d] = row
        return carry

    lax.fori_loop(0, n_seq, find, 0)

    loads[0].wait()
    values = win_v[...].astype(F32).reshape(rows_dev * 2 * UNIT, e)
    normed = (values * rms_scaling(values) * egain[...]).astype(BF16)
    loads[1].wait()
    pre = dot(normed, w_in_v[...])
    hidden = (pre * sigmoid(pre)).astype(BF16)
    loads[2].wait()
    encoded = values + dot(hidden, w_out_v[...])
    enc[...] = encoded.reshape(rows_dev, 2, UNIT, e).astype(BF16)

    def stage(d, carry):
        outg[d] = enc[rows_s[d]]
        return carry

    lax.fori_loop(0, n_seq, stage, 0)
    recv[me] = outg[me]
    pl.semaphore_wait(barrier, greeted)

    plans = {n: seq_exchange(n_seq, n, outg, recv, a_send, a_recv) for n in (1, 2)}
    for n in (1, 2):
        @pl.when(c == n - 1)
        def _(n=n):
            plans[n][0]()

    size = min(128, q.shape[0])
    blocks = q.shape[0] // size
    loads[3].wait()
    loads[4].wait()

    def query(i, carry):
        at = pl.ds(pl.multiple_of(i * size, size), size)
        vals = tok_v[at, :].astype(F32)
        unit = (vals * rms_scaling(vals) * dgain[...]).astype(BF16)
        q[at, :] = dot(unit, w_q_v[...]).astype(BF16)
        return carry

    lax.fori_loop(0, blocks, query, 0)
    loads[5].wait()
    loads[6].wait()

    def context_grad(i, carry):
        at = pl.ds(pl.multiple_of(i * size, size), size)
        where = me * q.shape[0] + i * size + lax.broadcasted_iota(jnp.int32, (size, 1), 0)
        live = lax.rem(where // STRETCH, SEQ_LEN // STRETCH) != 0
        grad = dot(gout_v[at, :], w_p_v[...], 1, 1)
        gctx[at, :] = jnp.where(live, grad, 0.0).astype(BF16)
        return carry

    lax.fori_loop(0, blocks, context_grad, 0)

    half = nb // 2
    right, left, opp = lax.rem(x + 1, nx), lax.rem(x + nx - 1, nx), lax.rem(x + 2, nx)
    for n in (1, 2):
        @pl.when(c == n - 1)
        def _(n=n):
            plans[n][1]()
            other = 3 - n

            def mine(xx, n=n):
                return full.at[:, pl.ds(3 * xx + n - 1, n)]

            def part(xx, h, n=n):
                return full.at[pl.ds(half * h, half), pl.ds(3 * xx + n - 1, n)]

            def pick(j, carry):
                slot = codes[me * nb + j] // rows_dev
                for i in range(n):
                    full[j, 3 * x + n - 1 + i] = recv[slot, i]
                return carry

            lax.fori_loop(0, nb, pick, 0)
            moved = []

            def send(i, ref, **where):
                copy = rcopy(ref, ref, b_send.at[i], b_recv.at[i], **where)
                copy.start()
                moved.append(copy)

            def got(i, ref, **where):
                rcopy(ref, ref, b_send.at[i], b_recv.at[i], **where).wait_recv()

            send(0, mine(x), mp_0=right)
            send(1, mine(x), mp_0=left)
            send(2, mine(x), mp_1=1 - c)
            got(0, mine(left), mp_0=left)
            send(3, part(left, 0), mp_0=right)
            send(4, mine(left), mp_1=1 - c)
            got(1, mine(right), mp_0=right)
            send(5, part(right, 1), mp_0=left)
            send(6, mine(right), mp_1=1 - c)
            got(3, part(opp, 0), mp_0=left)
            send(7, part(opp, 0), mp_1=1 - c)
            got(5, part(opp, 1), mp_0=right)
            send(8, part(opp, 1), mp_1=1 - c)
            got(2, mine(x, other), mp_1=1 - c)
            got(4, mine(left, other), mp_1=1 - c)
            got(6, mine(right, other), mp_1=1 - c)
            got(7, part(opp, 0, other), mp_1=1 - c)
            got(8, part(opp, 1, other), mp_1=1 - c)
            for copy in moved:
                copy.wait_send()
            plans[n][2]()


def fetch(dims, codes, db, egain, w_in, w_out, tok, gout, dgain, w_q, w_p):
    n_seq, nx, nb, rows_dev, e = dims
    slot = (2, UNIT, e)
    return pl.pallas_call(
        functools.partial(fetch_kernel, dims),
        out_shape=(
            jax.ShapeDtypeStruct((nb, db.shape[1], UNIT, e), BF16),
            jax.ShapeDtypeStruct((tok.shape[0], w_q.shape[1]), BF16),
            jax.ShapeDtypeStruct((tok.shape[0], w_q.shape[1]), BF16),
        ),
        in_specs=[SM, HB, VM, HB, HB, HB, HB, VM, HB, HB],
        out_specs=(VM, VM, VM),
        scratch_shapes=[
            pltpu.VMEM((rows_dev, *slot), BF16),
            pltpu.VMEM(w_in.shape, BF16),
            pltpu.VMEM(w_out.shape, BF16),
            pltpu.VMEM(tok.shape, BF16),
            pltpu.VMEM(gout.shape, BF16),
            pltpu.VMEM(w_q.shape, BF16),
            pltpu.VMEM(w_p.shape, BF16),
            pltpu.VMEM((rows_dev, *slot), BF16),
            pltpu.VMEM((n_seq, *slot), BF16),
            pltpu.VMEM((n_seq, *slot), BF16),
            pltpu.SMEM((n_seq,), jnp.int32),
            pltpu.SemaphoreType.DMA((7,)),
            pltpu.SemaphoreType.DMA((n_seq,)),
            pltpu.SemaphoreType.DMA((n_seq,)),
            pltpu.SemaphoreType.DMA((9,)),
            pltpu.SemaphoreType.DMA((9,)),
        ],
        compiler_params=pltpu.CompilerParams(
            collective_id=0, has_side_effects=True, vmem_limit_bytes=BIG
        ),
        name="fetch",
    )(codes, db, egain, w_in, w_out, tok, gout, dgain, w_q, w_p)


def attend_kernel(per, full, q, gctx, w_k, w_v, terms, ctx, dq):
    heads = q.shape[1] // HD
    span = full.shape[0] // per
    factor = HD ** (-0.5)
    keys, vals = [], []
    for s in range(per):
        rows = full[s * span:(s + 1) * span, :]
        keys.append(dot(rows, w_k[...]).astype(BF16))
        vals.append(dot(rows, w_v[...]).astype(BF16))
    todo = [(s, h) for s in range(per) for h in range(heads)]
    at = {
        (s, h): (slice(s * STRETCH, (s + 1) * STRETCH), slice(h * HD, (h + 1) * HD))
        for s, h in todo
    }
    qs = {t: q[at[t]] for t in todo}
    gs = {t: gctx[at[t]] for t in todo}
    ks = {(s, h): keys[s][:, h * HD:(h + 1) * HD] for s, h in todo}
    vs = {(s, h): vals[s][:, h * HD:(h + 1) * HD] for s, h in todo}
    exps = {t: jnp.exp(dot(qs[t], ks[t], 1, 1) * factor) for t in todo}
    dps = {t: dot(gs[t], vs[t], 1, 1) for t in todo}
    probs = {t: exps[t] / jnp.sum(exps[t], axis=-1, keepdims=True) for t in todo}
    weights = {t: probs[t].astype(BF16) for t in todo}
    scores = {
        t: (
            probs[t] * (dps[t] - jnp.sum(probs[t] * dps[t], axis=-1, keepdims=True)) * factor
        ).astype(BF16)
        for t in todo
    }
    for t in todo:
        ctx[at[t]] = dot(weights[t], vs[t]).astype(BF16)
        dq[at[t]] = dot(scores[t], ks[t]).astype(BF16)
    dks = {t: dot(scores[t], qs[t], 0, 0).astype(BF16) for t in todo}
    dvs = {t: dot(weights[t], gs[t], 0, 0).astype(BF16) for t in todo}
    for s in range(per):
        dk = jnp.concatenate([dks[(s, h)] for h in range(heads)], axis=1)
        dv = jnp.concatenate([dvs[(s, h)] for h in range(heads)], axis=1)
        out = dot(dk, w_k[...], 1, 1) + dot(dv, w_v[...], 1, 1)
        terms[s * span:(s + 1) * span, :] = out.astype(BF16)


def attend(full, q, gctx, w_k, w_v, per):
    steps = q.shape[0] // STRETCH // per
    rows, e = full.shape
    width = q.shape[1]

    def cut(r, w):
        return pl.BlockSpec((r // steps, w), lambda i: (i, 0))

    def whole(a):
        return pl.BlockSpec(a.shape, lambda i: (0, 0))

    return pl.pallas_call(
        functools.partial(attend_kernel, per),
        grid=(steps,),
        out_shape=(
            jax.ShapeDtypeStruct(full.shape, BF16),
            jax.ShapeDtypeStruct(q.shape, BF16),
            jax.ShapeDtypeStruct(q.shape, BF16),
        ),
        in_specs=[cut(rows, e), cut(q.shape[0], width), cut(q.shape[0], width), whole(w_k), whole(w_v)],
        out_specs=(cut(rows, e), cut(q.shape[0], width), cut(q.shape[0], width)),
        compiler_params=pltpu.CompilerParams(vmem_limit_bytes=BIG),
        name="attend",
    )(full, q, gctx, w_k, w_v)


def return_kernel(
    dims,
    codes, terms, ctx, dq, tok, dgain, w_q, w_p,
    recv, own, fin,
    sib, relay, last, comb, ge, back, gn, outs, osib, orelay, ocomb, pick_s,
    d_send, d_recv, o_send, o_recv, e_send, e_recv, f_send, f_recv,
):
    n_seq, nx, nb, rows_dev, e = dims
    me, x, c = lax.axis_index("seq"), lax.axis_index("mp_0"), lax.axis_index("mp_1")
    barrier, greeted = greet(n_seq, nx)
    half = nb // 2
    right, left, opp = lax.rem(x + 1, nx), lax.rem(x + nx - 1, nx), lax.rem(x + 2, nx)
    branches = (1, 2)

    def each(f):
        for n in branches:
            @pl.when(c == n - 1)
            def _(n=n):
                f(n)

    def pairs(n):
        other = 3 - n
        return [
            (
                rcopy(
                    terms.at[:, pl.ds(3 * k + other - 1, other)],
                    sib.at[k, :, pl.ds(0, other)],
                    d_send.at[k],
                    d_recv.at[k],
                    mp_1=1 - c,
                ),
                rcopy(
                    terms.at[:, pl.ds(3 * k + n - 1, n)],
                    sib.at[k, :, pl.ds(0, n)],
                    d_send.at[k],
                    d_recv.at[k],
                    mp_1=1 - c,
                ),
            )
            for k in range(nx)
        ]

    def find(s, carry):
        spot = jnp.int32(0)
        for k in range(nb):
            spot = jnp.where(codes[me * nb + k] // rows_dev == s, k, spot)
        pick_s[s] = spot
        return carry

    lax.fori_loop(0, n_seq, find, 0)
    pl.semaphore_wait(barrier, greeted)

    def pair_start(n):
        for sent, _ in pairs(n):
            sent.start()

    each(pair_start)

    rows = ctx.shape[0]
    lanes = 2 * nx
    cols = tok.shape[2]
    live = lax.rem(
        (me * rows + lax.broadcasted_iota(jnp.int32, (rows, 1), 0)) // STRETCH, SEQ_LEN // STRETCH
    ) != 0

    def squares(l, total):
        vals = tok[l].astype(F32)
        return total + jnp.sum(vals * vals, axis=-1, keepdims=True)

    scaling = lax.rsqrt(
        lax.fori_loop(0, lanes, squares, jnp.zeros((rows, 1), F32)) / (lanes * cols) + EPSILON
    )

    def forward(l, total):
        out = dot(ctx[...], w_p[l])
        outs[l // 2, lax.rem(l, 2), 0] = jnp.where(live, out, 0.0).astype(BF16)
        grad = dot(dq[...], w_q[l], 1, 1) * dgain[l]
        gn[l] = grad
        return total + jnp.sum(grad * tok[l].astype(F32), axis=-1, keepdims=True)

    total = lax.fori_loop(0, lanes, forward, jnp.zeros((rows, 1), F32))
    slope = total * scaling * scaling / (lanes * cols)

    def finish(l, carry):
        grad = scaling * (gn[l] - tok[l].astype(F32) * slope)
        outs[l // 2, lax.rem(l, 2), 1] = grad.astype(BF16)
        return carry

    lax.fori_loop(0, lanes, finish, 0)

    def reduce_first(n):
        for (_, got), k in zip(pairs(n), range(nx)):
            got.wait_recv()

        def add(i, carry):
            k, j = i // nb, lax.rem(i, nb)
            for u in range(n):
                comb[k, j, u] = (
                    terms[j, 3 * k + n - 1 + u].astype(F32) + sib[k, j, u].astype(F32)
                ).astype(BF16)
            return carry

        lax.fori_loop(0, nx * nb, add, 0)

    each(reduce_first)

    def relays(n):
        return [
            rcopy(
                comb.at[opp, pl.ds(half * h, half), pl.ds(0, n)],
                relay.at[h, :, pl.ds(0, n)],
                d_send.at[nx + h],
                d_recv.at[nx + h],
                mp_0=to,
            )
            for h, to in ((0, right), (1, left))
        ]

    def ends(n):
        return [
            rcopy(
                comb.at[to, :, pl.ds(0, n)],
                last.at[h, :, pl.ds(0, n)],
                d_send.at[nx + 2 + h],
                d_recv.at[nx + 2 + h],
                mp_0=to,
            )
            for h, to in ((0, right), (1, left))
        ]

    def relay_start(n):
        for copy in relays(n):
            copy.start()

    each(relay_start)

    def out_pair():
        return [
            rcopy(outs.at[k, 1 - c], osib.at[k], o_send.at[k], o_recv.at[k], mp_1=1 - c)
            for k in range(nx)
        ]

    for copy in out_pair():
        copy.start()

    def relay_end(n):
        for h, copy in enumerate(relays(n)):
            copy.wait_recv()

        for h, to in ((0, right), (1, left)):

            def add(j, carry, h=h, to=to):
                for u in range(n):
                    comb[to, half * h + j, u] = (
                        comb[to, half * h + j, u].astype(F32) + relay[h, j, u].astype(F32)
                    ).astype(BF16)
                return carry

            lax.fori_loop(0, half, add, 0)
        for copy in ends(n):
            copy.start()

    each(relay_end)

    for k, copy in enumerate(out_pair()):
        copy.wait_recv()

        def add(i, carry, k=k):
            at = pl.ds(pl.multiple_of(i * STRETCH, STRETCH), STRETCH)
            for t in range(2):
                ocomb[k, t, at, :] = (
                    outs[k, c, t, at, :].astype(F32) + osib[k, t, at, :].astype(F32)
                ).astype(BF16)
            return carry

        lax.fori_loop(0, rows // STRETCH, add, 0)
    own[...] = ocomb[x]

    def out_relays():
        return [
            rcopy(ocomb.at[opp, h], orelay.at[h], o_send.at[nx + h], o_recv.at[nx + h], mp_0=to)
            for h, to in ((0, right), (1, left))
        ]

    def out_ends():
        return [
            rcopy(ocomb.at[to], fin.at[h], o_send.at[nx + 2 + h], o_recv.at[nx + 2 + h], mp_0=to)
            for h, to in ((0, right), (1, left))
        ]

    for copy in out_relays():
        copy.start()

    plans = {n: seq_exchange(n_seq, n, back, recv, e_send, e_recv) for n in branches}

    def give_back(n):
        for copy in ends(n):
            copy.wait_recv()

        def add(j, carry):
            for u in range(n):
                ge[j, u] = (
                    comb[x, j, u].astype(F32)
                    + last[0, j, u].astype(F32)
                    + last[1, j, u].astype(F32)
                ).astype(BF16)
            return carry

        lax.fori_loop(0, nb, add, 0)

        def stage(s, carry):
            spot = pick_s[s]
            for u in range(n):
                back[s, u] = ge[spot, u]
            return carry

        lax.fori_loop(0, n_seq, stage, 0)
        for u in range(n):
            recv[me, u] = back[me, u]
        plans[n][0]()

    each(give_back)

    for h, (copy, to) in enumerate(zip(out_relays(), (right, left))):
        copy.wait_recv()

        def add(i, carry, h=h, to=to):
            at = pl.ds(pl.multiple_of(i * STRETCH, STRETCH), STRETCH)
            ocomb[to, h, at, :] = (
                ocomb[to, h, at, :].astype(F32) + orelay[h, at, :].astype(F32)
            ).astype(BF16)
            return carry

        lax.fori_loop(0, rows // STRETCH, add, 0)
    for copy in out_ends():
        copy.start()

    shared = rcopy(recv.at[:, 0], recv.at[:, 1], f_send, f_recv, mp_1=1 - c)

    def settle(n):
        plans[n][1]()
        if n == 2:
            shared.start()
        else:
            shared.wait_recv()
        plans[n][2]()
        for sent, _ in pairs(n):
            sent.wait_send()
        for copy in relays(n) + ends(n):
            copy.wait_send()
        if n == 2:
            shared.wait_send()

    each(settle)
    for copy in out_ends():
        copy.wait_recv()
    for copy in out_pair() + out_relays() + out_ends():
        copy.wait_send()


def give(dims, codes, terms, ctx, dq, tok, dgain, w_q, w_p):
    n_seq, nx, nb, rows_dev, e = dims
    rows = ctx.shape[0]
    lanes, _, cols = tok.shape
    half = nb // 2
    slot = (2, UNIT, e)
    return pl.pallas_call(
        functools.partial(return_kernel, dims),
        out_shape=(
            jax.ShapeDtypeStruct((n_seq, *slot), BF16),
            jax.ShapeDtypeStruct((2, rows, cols), BF16),
            jax.ShapeDtypeStruct((2, 2, rows, cols), BF16),
        ),
        in_specs=[SM] + [VM] * 7,
        out_specs=(VM, VM, VM),
        scratch_shapes=[
            pltpu.VMEM((nx, nb, *slot), BF16),
            pltpu.VMEM((2, half, *slot), BF16),
            pltpu.VMEM((2, nb, *slot), BF16),
            pltpu.VMEM((nx, nb, *slot), BF16),
            pltpu.VMEM((nb, *slot), BF16),
            pltpu.VMEM((n_seq, *slot), BF16),
            pltpu.VMEM((lanes, rows, cols), F32),
            pltpu.VMEM((nx, 2, 2, rows, cols), BF16),
            pltpu.VMEM((nx, 2, rows, cols), BF16),
            pltpu.VMEM((2, rows, cols), BF16),
            pltpu.VMEM((nx, 2, rows, cols), BF16),
            pltpu.SMEM((n_seq,), jnp.int32),
            pltpu.SemaphoreType.DMA((nx + 4,)),
            pltpu.SemaphoreType.DMA((nx + 4,)),
            pltpu.SemaphoreType.DMA((nx + 4,)),
            pltpu.SemaphoreType.DMA((nx + 4,)),
            pltpu.SemaphoreType.DMA((n_seq,)),
            pltpu.SemaphoreType.DMA((n_seq,)),
            pltpu.SemaphoreType.DMA,
            pltpu.SemaphoreType.DMA,
        ],
        compiler_params=pltpu.CompilerParams(
            collective_id=1, has_side_effects=True, vmem_limit_bytes=BIG
        ),
        name="give",
    )(codes, terms, ctx, dq, tok, dgain, w_q, w_p)


def settle_kernel(dims, codes, recv, own, fin, db, egain, w_in, w_out, cca, gtok, gdb, win_v, acc, lsem):
    n_seq, nx, nb, rows_dev, e = dims
    me, x, c = lax.axis_index("seq"), lax.axis_index("mp_0"), lax.axis_index("mp_1")
    load = pltpu.make_async_copy(db.at[:, pl.ds(3 * x + c, 2)], win_v, lsem)
    load.start()
    cca[...] = (own[0].astype(F32) + fin[0, 0].astype(F32) + fin[1, 0].astype(F32)).astype(BF16)
    gtok[...] = own[1].astype(F32) + fin[0, 1].astype(F32) + fin[1, 1].astype(F32)
    acc[...] = jnp.zeros_like(acc)

    def gather(d, carry):
        for k in range(nb):
            code = codes[d * nb + k]

            @pl.when(code // rows_dev == me)
            def _():
                r = lax.rem(code, rows_dev)
                acc[r] = acc[r] + recv[d].astype(F32)

        return carry

    lax.fori_loop(0, n_seq, gather, 0)
    grad_enc = acc[...].reshape(rows_dev * 2 * UNIT, e)
    load.wait()
    values = win_v[...].astype(F32).reshape(rows_dev * 2 * UNIT, e)
    scaling = rms_scaling(values)
    unit = values * scaling
    pre = dot((unit * egain[...]).astype(BF16), w_in[...])
    s = sigmoid(pre)
    grad_hidden = dot(grad_enc.astype(BF16), w_out[...], 1, 1)
    grad_pre = (grad_hidden * (s * (1.0 + pre * (1.0 - s)))).astype(BF16)
    g = dot(grad_pre, w_in[...], 1, 1) * egain[...]
    out = grad_enc + scaling * (g - unit * jnp.mean(g * unit, axis=-1, keepdims=True))
    out = out.reshape(rows_dev, 2 * UNIT, e)
    keep = gdb.shape[1]
    for n in range(2):
        @pl.when(c == n)
        def _(n=n):
            gdb[...] = out[:, (2 * UNIT - keep) * n:(2 * UNIT - keep) * n + keep, :]


def settle(dims, codes, recv, own, fin, db, egain, w_in, w_out):
    n_seq, nx, nb, rows_dev, e = dims
    return pl.pallas_call(
        functools.partial(settle_kernel, dims),
        out_shape=(
            jax.ShapeDtypeStruct(own.shape[1:], BF16),
            jax.ShapeDtypeStruct(own.shape[1:], F32),
            jax.ShapeDtypeStruct((rows_dev, 3 * UNIT // 2, e), F32),
        ),
        in_specs=[SM, VM, VM, VM, HB, VM, VM, VM],
        out_specs=(VM, VM, VM),
        scratch_shapes=[
            pltpu.VMEM((rows_dev, 2, UNIT, e), BF16),
            pltpu.VMEM((rows_dev, 2, UNIT, e), F32),
            pltpu.SemaphoreType.DMA,
        ],
        compiler_params=pltpu.CompilerParams(vmem_limit_bytes=BIG),
        name="settle",
    )(codes, recv, own, fin, db, egain, w_in, w_out)


def body(
    n_seq, nx,
    tokens, database, nb_shard, nb_row, dec_gain, enc_gain,
    w_in, w_out, w_query, w_key, w_value, w_proj, grad_out,
):
    rows_dev, length, e = database.shape
    rows, d = tokens.shape
    width = w_query.shape[1]
    nb = rows // STRETCH * K
    lanes = 2 * nx
    dims = (n_seq, nx, nb, rows_dev, e)
    codes = (nb_shard * rows_dev + nb_row).reshape(-1)
    db = database.reshape(rows_dev, length // UNIT, UNIT, e)
    egain = enc_gain.reshape(1, e)
    full, q, gctx = fetch(
        dims, codes, db, egain, w_in, w_out, tokens, grad_out, dec_gain.reshape(1, d), w_query, w_proj
    )
    terms, ctx, dq = attend(
        full.reshape(nb * length, e), q, gctx, w_key, w_value, max(1, nb // K // 2)
    )
    tok = tokens.reshape(rows, lanes, d // lanes).transpose(1, 0, 2)
    w_p = w_proj.reshape(width, lanes, d // lanes).transpose(1, 0, 2)
    w_q = w_query.reshape(lanes, d // lanes, width)
    recv, own, fin = give(
        dims, codes, terms.reshape(full.shape), ctx, dq, tok, dec_gain.reshape(lanes, 1, d // lanes), w_q, w_p
    )
    return settle(dims, codes, recv, own, fin, db, egain, w_in, w_out)


def solution(mesh):
    n_seq = mesh.shape["seq"]
    nx = mesh.shape["mp"] // 2
    split = Mesh(mesh.devices.reshape(n_seq, nx, 2), ("seq", "mp_0", "mp_1"))
    placed = (
        P("seq", None),
        P("seq", None, None),
        P(),
        P(),
        P(),
        P(),
        P(),
        P(),
        P(None, MP),
        P(None, MP),
        P(None, MP),
        P(MP, None),
        P("seq", None),
    )
    return jax.shard_map(
        functools.partial(body, n_seq, nx),
        mesh=split,
        in_specs=placed,
        out_specs=(P("seq", MP), P("seq", MP), P("seq", MP, None)),
        check_vma=False,
    )
```

```python
import functools

import jax
import jax.numpy as jnp
from jax import lax
from jax.experimental import pallas as pl
from jax.experimental.pallas import tpu as pltpu
from jax.sharding import Mesh
from jax.sharding import PartitionSpec as P

HD = 128
STRETCH = 64
K = 2
SEQ_LEN = 4096
UNIT = 8
EPSILON = 1e-06
MP = ("mp_0", "mp_1")
F32 = jnp.float32
BF16 = jnp.bfloat16
VM = pl.BlockSpec(memory_space=pltpu.VMEM)
SM = pl.BlockSpec(memory_space=pltpu.SMEM)
HB = pl.BlockSpec(memory_space=pltpu.HBM)
BIG = 64000 * 1024
FORE = (4, 3)
AFT = (3, 4)


def rcopy(src, dst, ssem, rsem, **where):
    return pltpu.make_async_remote_copy(
        src_ref=src,
        dst_ref=dst,
        send_sem=ssem,
        recv_sem=rsem,
        device_id=where,
        device_id_type=pl.DeviceIdType.MESH,
    )


def dot(a, b, ca=1, cb=0):
    return lax.dot_general(a, b, (((ca,), (cb,)), ((), ())), preferred_element_type=F32)


def rms_scaling(values):
    return lax.rsqrt(jnp.mean(values * values, axis=-1, keepdims=True) + EPSILON)


def sigmoid(v):
    return 1.0 / (1.0 + jnp.exp(-v))


def greet(n_seq, nx):
    me, x, c = lax.axis_index("seq"), lax.axis_index("mp_0"), lax.axis_index("mp_1")
    barrier = pltpu.get_barrier_semaphore()

    def tell(**where):
        pl.semaphore_signal(barrier, inc=1, device_id=where, device_id_type=pl.DeviceIdType.MESH)

    def far(k, carry):
        tell(seq=lax.rem(me + k, n_seq))
        return carry

    lax.fori_loop(1, n_seq, far, 0)
    tell(mp_0=lax.rem(x + 1, nx))
    tell(mp_0=lax.rem(x + nx - 1, nx))
    tell(mp_1=1 - c)
    return barrier, n_seq + 2


def seq_exchange(n_seq, n, src, dst, send, recv, src_lanes=None):
    me = lax.axis_index("seq")

    def piece(k, sending):
        peer = lax.rem(me + k, n_seq) if sending else lax.rem(me + n_seq - k, n_seq)
        at = me if sending else peer
        if src_lanes is None:
            a, b = src.at[peer, pl.ds(0, n)], dst.at[at, pl.ds(0, n)]
        else:
            a, b = src.at[peer, pl.ds(0, n), :, src_lanes], dst.at[at, pl.ds(0, n)]
        return rcopy(a, b, send.at[peer], recv.at[at], seq=peer)

    def run(sending, act):
        def go(k, carry):
            act(piece(k, sending))
            return carry

        lax.fori_loop(1, n_seq, go, 0)

    return (
        lambda: run(True, lambda copy: copy.start()),
        lambda: run(False, lambda copy: copy.wait_recv()),
        lambda: run(True, lambda copy: copy.wait_send()),
    )


def cuts(e, sizes):
    tiles = e // 128
    at, out = 0, []
    for i, share in enumerate(sizes):
        wide = tiles - at if i == len(sizes) - 1 else max(1, tiles * share // sum(sizes))
        out.append((at * 128, wide * 128))
        at += wide
    return out


def loop(count, f):
    def go(i, carry):
        f(i)
        return carry

    lax.fori_loop(0, count, go, 0)


def step_kernel(
    dims,
    shards, rows_in, db, egain, w_in, w_out, tok, gout, dgain, w_q, w_p, w_k, w_v,
    cca, gtok, gdb,
    win_v, w_in_v, w_out_v, tok_v, gout_v, w_q_v, w_p_v, w_k_v, w_v_v,
    enc, slope, outg, recvs, full, q, gctx, tscale, kv, ctx, dq, dkv,
    terms, sib, relay, last, comb, ge, back, got_back, acc, grad_hid,
    gn, outs, osib, orelay, ocomb, fin,
    rows_s, name_s, pick_s,
    lsem, a_send, a_recv, b_send, b_recv, d_send, d_recv, o_send, o_recv, e_send, e_recv, f_send, f_recv,
):
    n_seq, nx, nb, rows_dev, e, fore, aft = dims
    me, x, c = lax.axis_index("seq"), lax.axis_index("mp_0"), lax.axis_index("mp_1")
    barrier, greeted = greet(n_seq, nx)
    half = nb // 2
    per_dev = nb // K
    right, left, opp = lax.rem(x + 1, nx), lax.rem(x + nx - 1, nx), lax.rem(x + 2, nx)
    branches = (1, 2)

    def each(f, *args):
        for n in branches:
            @pl.when(c == n - 1)
            def _(n=n):
                f(n, *args)

    loads = [
        pltpu.make_async_copy(s, d, lsem.at[i])
        for i, (s, d) in enumerate(
            (
                (db.at[:, pl.ds(3 * x + c, 2)], win_v),
                (w_in, w_in_v),
                (w_out, w_out_v),
                (tok, tok_v),
                (w_q, w_q_v),
                (gout, gout_v),
                (w_p, w_p_v),
                (w_k, w_k_v),
                (w_v, w_v_v),
            )
        )
    ]
    for load in loads:
        load.start()

    def find(d):
        row, named = jnp.int32(0), jnp.int32(-1)
        for k in range(nb):
            hit = shards[k % K, d * per_dev + k // K] == me
            at = rows_in[k % K, d * per_dev + k // K]
            row, named = jnp.where(hit, at, row), jnp.where(hit, at, named)
        rows_s[d] = row
        name_s[d] = named

    loop(n_seq, find)

    units = rows_dev * 2 * UNIT
    loads[0].wait()
    values = win_v[...].astype(F32).reshape(units, e)
    gain = egain[...].reshape(1, e)
    normed = (values * rms_scaling(values) * gain).astype(BF16)
    loads[1].wait()
    pre = dot(normed, w_in_v[...])
    gate = sigmoid(pre)
    slope[...] = gate * (1.0 + pre * (1.0 - gate))
    hidden = (pre * gate).astype(BF16)
    loads[2].wait()
    encoded = values + dot(hidden, w_out_v[...])
    enc[...] = encoded.reshape(rows_dev, 2, UNIT, e).astype(BF16)

    def stage_out(d):
        outg[d] = enc[rows_s[d]]

    loop(n_seq, stage_out)
    for (l0, w), recv in zip(fore, recvs):
        recv[me] = outg[me, :, :, l0:l0 + w]
    pl.semaphore_wait(barrier, greeted)

    ask = {
        n: [
            seq_exchange(n_seq, n, outg, recv, a_send.at[i], a_recv.at[i], pl.ds(l0, w))
            for i, ((l0, w), recv) in enumerate(zip(fore, recvs))
        ]
        for n in branches
    }

    def ask_start(n):
        for plan in ask[n]:
            plan[0]()

    each(ask_start)

    size = min(128, q.shape[0])
    blocks = q.shape[0] // size
    loads[3].wait()
    loads[4].wait()

    def query(i):
        at = pl.ds(pl.multiple_of(i * size, size), size)
        vals = tok_v[at, :].astype(F32)
        scale = rms_scaling(vals)
        tscale[at, :] = scale
        q[at, :] = dot((vals * scale * dgain[...]).astype(BF16), w_q_v[...]).astype(BF16)

    loop(blocks, query)
    loads[5].wait()
    loads[6].wait()

    def context_grad(i):
        at = pl.ds(pl.multiple_of(i * size, size), size)
        where = me * q.shape[0] + i * size + lax.broadcasted_iota(jnp.int32, (size, 1), 0)
        alive = lax.rem(where // STRETCH, SEQ_LEN // STRETCH) != 0
        grad = dot(gout_v[at, :], w_p_v[...], 1, 1)
        gctx[at, :] = jnp.where(alive, grad, 0.0).astype(BF16)

    loop(blocks, context_grad)
    loads[7].wait()
    loads[8].wait()

    def mine(n, i, xx):
        l0, w = fore[i]
        return full.at[:, pl.ds(3 * xx + n - 1, n), :, pl.ds(l0, w)]

    def part(n, i, xx, h):
        l0, w = fore[i]
        return full.at[pl.ds(half * h, half), pl.ds(3 * xx + n - 1, n), :, pl.ds(l0, w)]

    def ring(n, i, k, ref, **where):
        return rcopy(ref, ref, b_send.at[i, k], b_recv.at[i, k], **where)

    def ring_copies(n, i):
        sib_to = dict(mp_1=1 - c)
        return [
            ring(n, i, 0, part(n, i, x, 0), mp_0=right),
            ring(n, i, 1, part(n, i, x, 1), mp_0=left),
            ring(n, i, 2, part(n, i, x, 1), mp_0=right),
            ring(n, i, 3, part(n, i, x, 0), mp_0=left),
            ring(n, i, 4, mine(n, i, x), **sib_to),
            ring(n, i, 5, part(n, i, left, 0), mp_0=right),
            ring(n, i, 6, part(n, i, right, 1), mp_0=left),
            ring(n, i, 7, mine(n, i, left), **sib_to),
            ring(n, i, 8, mine(n, i, right), **sib_to),
            ring(n, i, 9, part(n, i, opp, 0), **sib_to),
            ring(n, i, 10, part(n, i, opp, 1), **sib_to),
        ]

    def ring_got(n, i, k):
        ref = {
            0: lambda: part(n, i, left, 0),
            1: lambda: part(n, i, right, 1),
            2: lambda: part(n, i, left, 1),
            3: lambda: part(n, i, right, 0),
            4: lambda: mine(n, i, x),
            5: lambda: part(n, i, opp, 0),
            6: lambda: part(n, i, opp, 1),
            7: lambda: mine(n, i, left),
            8: lambda: mine(n, i, right),
            9: lambda: part(n, i, opp, 0),
            10: lambda: part(n, i, opp, 1),
        }[k]()
        ring(n, i, k, ref, mp_1=1 - c).wait_recv()

    def ring_open(n, i):
        ask[n][i][1]()
        l0, w = fore[i]

        def pick(j):
            slot = shards[lax.rem(j, K), me * per_dev + j // K]
            for u in range(n):
                full[j, 3 * x + n - 1 + u, :, l0:l0 + w] = recvs[i][slot, u]

        loop(nb, pick)
        for copy in ring_copies(n, i)[:5]:
            copy.start()

    def ring_pass(n, i):
        copies = ring_copies(n, i)
        ring_got(n, i, 0)
        copies[5].start()
        ring_got(n, i, 1)
        copies[6].start()
        ring_got(n, i, 2)
        copies[7].start()
        ring_got(n, i, 3)
        copies[8].start()

    def ring_close(n, i):
        copies = ring_copies(n, i)
        ring_got(n, i, 5)
        copies[9].start()
        ring_got(n, i, 6)
        copies[10].start()
        for k in (4, 7, 8, 9, 10):
            ring_got(3 - n, i, k)

    span = K * 12 * UNIT * nx // 4
    many = max(1, per_dev // 2)
    turns = per_dev // many
    tall = many * span

    def project(i):
        l0, w = fore[i]

        def go(t):
            at = pl.ds(pl.multiple_of(t * tall, tall), tall)
            rows = full[pl.ds(t * many * K, many * K), :, :, l0:l0 + w]
            rows = rows.astype(F32).reshape(tall, w).astype(BF16)
            for h, weight in enumerate((w_k_v, w_v_v)):
                out = dot(rows, weight[l0:l0 + w, :])
                if i:
                    out = out + kv[h, at, :]
                kv[h, at, :] = out

        loop(turns, go)

    each(ring_open, 0)
    for i in range(1, len(fore)):
        each(ring_pass, i - 1)
        each(ring_open, i)
        each(ring_close, i - 1)
        project(i - 1)
    each(ring_pass, len(fore) - 1)
    each(ring_close, len(fore) - 1)
    project(len(fore) - 1)

    width = q.shape[1]
    heads = width // HD
    factor = HD ** (-0.5)

    def attend(t):
        at = pl.ds(pl.multiple_of(t * tall, tall), tall)
        here = pl.ds(pl.multiple_of(t * many * STRETCH, many * STRETCH), many * STRETCH)
        todo = [(s, h) for s in range(many) for h in range(heads)]

        def pieces(block, high):
            return {
                (s, h): block[s * high:(s + 1) * high, h * HD:(h + 1) * HD] for s, h in todo
            }

        qs, gs = pieces(q[here, :], STRETCH), pieces(gctx[here, :], STRETCH)
        ks, vs = pieces(kv[0, at, :].astype(BF16), span), pieces(kv[1, at, :].astype(BF16), span)
        exps = {p: jnp.exp(dot(qs[p], ks[p], 1, 1) * factor) for p in todo}
        dps = {p: dot(gs[p], vs[p], 1, 1) for p in todo}
        probs = {p: exps[p] / jnp.sum(exps[p], axis=-1, keepdims=True) for p in todo}
        weights = {p: probs[p].astype(BF16) for p in todo}
        scores = {
            p: (
                probs[p] * (dps[p] - jnp.sum(probs[p] * dps[p], axis=-1, keepdims=True)) * factor
            ).astype(BF16)
            for p in todo
        }
        for s in range(many):
            lines = pl.ds(pl.multiple_of((t * many + s) * STRETCH, STRETCH), STRETCH)
            ends = pl.ds(pl.multiple_of((t * many + s) * span, span), span)
            for h in range(heads):
                p, lanes = (s, h), slice(h * HD, (h + 1) * HD)
                ctx[lines, lanes] = dot(weights[p], vs[p]).astype(BF16)
                dq[lines, lanes] = dot(scores[p], ks[p]).astype(BF16)
                dkv[0, ends, lanes] = dot(scores[p], qs[p], 0, 0).astype(BF16)
                dkv[1, ends, lanes] = dot(weights[p], gs[p], 0, 0).astype(BF16)

    loop(turns, attend)

    def lanes_of(i):
        l0, w = aft[i]
        return pl.ds(l0, w)

    def pair_copy(n, i, k, m):
        return rcopy(
            terms.at[:, pl.ds(3 * k + m - 1, m), :, lanes_of(i)],
            sib.at[k, :, pl.ds(0, m), :, lanes_of(i)],
            d_send.at[i, k],
            d_recv.at[i, k],
            mp_1=1 - c,
        )

    def pair_start(n, i):
        for k in range(nx):
            pair_copy(n, i, k, 3 - n).start()

    def relays(n, i):
        return [
            rcopy(
                comb.at[opp, pl.ds(half * h, half), pl.ds(0, n), :, lanes_of(i)],
                relay.at[h, :, pl.ds(0, n), :, lanes_of(i)],
                d_send.at[i, nx + h],
                d_recv.at[i, nx + h],
                mp_0=to,
            )
            for h, to in ((0, right), (1, left))
        ]

    def ends(n, i):
        return [
            rcopy(
                comb.at[to, :, pl.ds(0, n), :, lanes_of(i)],
                last.at[h, :, pl.ds(0, n), :, lanes_of(i)],
                d_send.at[i, nx + 2 + h],
                d_recv.at[i, nx + 2 + h],
                mp_0=to,
            )
            for h, to in ((0, right), (1, left))
        ]

    def reduce_pair(n, i):
        l0, w = aft[i]
        for k in range(nx):
            pair_copy(n, i, k, n).wait_recv()

        def add(k, j):
            for u in range(n):
                comb[k, j, u, :, l0:l0 + w] = (
                    terms[j, 3 * k + n - 1 + u, :, l0:l0 + w].astype(F32)
                    + sib[k, j, u, :, l0:l0 + w].astype(F32)
                ).astype(BF16)

        loop(nb, lambda j: add(opp, j))
        for copy in relays(n, i):
            copy.start()
        for k in (right, left, x):
            loop(nb, lambda j, k=k: add(k, j))

    def reduce_ends(n, i):
        l0, w = aft[i]
        for h, (copy, to) in enumerate(zip(relays(n, i), (right, left))):
            copy.wait_recv()

            def add(j, h=h, to=to):
                for u in range(n):
                    comb[to, half * h + j, u, :, l0:l0 + w] = (
                        comb[to, half * h + j, u, :, l0:l0 + w].astype(F32)
                        + relay[h, j, u, :, l0:l0 + w].astype(F32)
                    ).astype(BF16)

            loop(half, add)
            ends(n, i)[h].start()

    def give_back(n, i):
        l0, w = aft[i]
        for copy in ends(n, i):
            copy.wait_recv()

        def add(j):
            for u in range(n):
                ge[j, u, :, l0:l0 + w] = (
                    comb[x, j, u, :, l0:l0 + w].astype(F32)
                    + last[0, j, u, :, l0:l0 + w].astype(F32)
                    + last[1, j, u, :, l0:l0 + w].astype(F32)
                ).astype(BF16)

        loop(nb, add)

        def stage(s):
            spot = pick_s[s]
            for u in range(n):
                back[i][s, u] = ge[spot, u, :, l0:l0 + w]

        loop(n_seq, stage)
        for u in range(n):
            got_back[i][me, u] = back[i][me, u]
        returns[n][i][0]()

    returns = {
        n: [
            seq_exchange(n_seq, n, back[i], got_back[i], e_send.at[i], e_recv.at[i])
            for i in range(len(aft))
        ]
        for n in branches
    }

    def shared(i):
        return rcopy(
            got_back[i].at[:, 0], got_back[i].at[:, 1], f_send.at[i], f_recv.at[i], mp_1=1 - c
        )

    def terms_of(i):
        l0, w = aft[i]

        def go(t):
            at = pl.ds(pl.multiple_of(t * tall, tall), tall)
            out = dot(dkv[0, at, :], w_k_v[l0:l0 + w, :], 1, 1)
            out = out + dot(dkv[1, at, :], w_v_v[l0:l0 + w, :], 1, 1)
            terms[pl.ds(t * many * K, many * K), :, :, l0:l0 + w] = out.reshape(
                many * K, 3 * nx, UNIT, w
            ).astype(BF16)

        loop(turns, go)

    def find_back(s):
        spot = jnp.int32(0)
        for k in range(nb):
            spot = jnp.where(shards[k % K, me * per_dev + k // K] == s, k, spot)
        pick_s[s] = spot

    high = ctx.shape[0]
    lanes = 2 * nx
    cols = tok_v.shape[1] // lanes
    live = lax.rem(
        (me * high + lax.broadcasted_iota(jnp.int32, (high, 1), 0)) // STRETCH, SEQ_LEN // STRETCH
    ) != 0

    def columns(l):
        return pl.ds(pl.multiple_of(l * cols, cols), cols)

    def out_terms():
        def forward(l, total):
            out = dot(ctx[...], w_p_v[:, columns(l)])
            outs[l // 2, lax.rem(l, 2), 0] = jnp.where(live, out, 0.0).astype(BF16)
            grad = dot(dq[...], w_q_v[columns(l), :], 1, 1) * dgain[:, columns(l)]
            gn[l] = grad
            return total + jnp.sum(
                grad * tok_v[:, columns(l)].astype(F32), axis=-1, keepdims=True
            )

        total = lax.fori_loop(0, lanes, forward, jnp.zeros((high, 1), F32))
        scale = tscale[...]
        tilt = total * scale * scale / (lanes * cols)

        def finish(l):
            grad = scale * (gn[l] - tok_v[:, columns(l)].astype(F32) * tilt)
            outs[l // 2, lax.rem(l, 2), 1] = grad.astype(BF16)

        loop(lanes, finish)

    def out_pair():
        return [
            rcopy(outs.at[k, 1 - c], osib.at[k], o_send.at[k], o_recv.at[k], mp_1=1 - c)
            for k in range(nx)
        ]

    def out_relays():
        return [
            rcopy(ocomb.at[opp, h], orelay.at[h], o_send.at[nx + h], o_recv.at[nx + h], mp_0=to)
            for h, to in ((0, right), (1, left))
        ]

    def out_ends():
        return [
            rcopy(ocomb.at[to], fin.at[h], o_send.at[nx + 2 + h], o_recv.at[nx + 2 + h], mp_0=to)
            for h, to in ((0, right), (1, left))
        ]

    def by_stretch(f):
        loop(high // STRETCH, lambda i: f(pl.ds(pl.multiple_of(i * STRETCH, STRETCH), STRETCH)))

    def out_reduce_pair():
        for copy in out_pair():
            copy.wait_recv()

        def add(k):
            def go(at):
                for t in range(2):
                    ocomb[k, t, at, :] = (
                        outs[k, c, t, at, :].astype(F32) + osib[k, t, at, :].astype(F32)
                    ).astype(BF16)

            by_stretch(go)

        add(opp)
        for copy in out_relays():
            copy.start()
        for k in (right, left, x):
            add(k)

    def out_reduce_ends():
        for h, (copy, to) in enumerate(zip(out_relays(), (right, left))):
            copy.wait_recv()

            def go(at, h=h, to=to):
                ocomb[to, h, at, :] = (
                    ocomb[to, h, at, :].astype(F32) + orelay[h, at, :].astype(F32)
                ).astype(BF16)

            by_stretch(go)
            out_ends()[h].start()

    def out_close():
        for copy in out_ends():
            copy.wait_recv()

        def go(at):
            def total(t):
                return (
                    ocomb[x, t, at, :].astype(F32)
                    + fin[0, t, at, :].astype(F32)
                    + fin[1, t, at, :].astype(F32)
                )

            cca[at, :] = total(0).astype(BF16)
            gtok[at, :] = total(1)

        by_stretch(go)

    for i in range(len(aft)):
        terms_of(i)
        each(pair_start, i)
    loop(n_seq, find_back)
    each(reduce_pair, 0)
    out_terms()
    for copy in out_pair():
        copy.start()
    for i in range(1, len(aft)):
        each(reduce_pair, i)
    each(reduce_ends, 0)
    out_reduce_pair()
    for i in range(1, len(aft)):
        each(reduce_ends, i)
    for i in range(len(aft)):
        each(give_back, i)
        if i == 0:
            out_reduce_ends()

    def collect(n, i):
        returns[n][i][1]()
        if n == 2:
            shared(i).start()
        else:
            shared(i).wait_recv()

    def tally(i):
        l0, w = aft[i]
        for u in range(2):
            def add(d, sums):
                named = name_s[d]
                slot = got_back[i][d, u].astype(F32)
                return tuple(
                    total + jnp.where(named == r, slot, 0.0) for r, total in enumerate(sums)
                )

            sums = lax.fori_loop(
                0, n_seq, add, tuple(jnp.zeros((UNIT, w), F32) for _ in range(rows_dev))
            )
            for r in range(rows_dev):
                acc[r, u, :, l0:l0 + w] = sums[r]
        part = acc[:, :, :, l0:l0 + w].reshape(units, w).astype(BF16)
        out = dot(part, w_out_v[:, l0:l0 + w], 1, 1)
        grad_hid[...] = out if i == 0 else grad_hid[...] + out

    for i in range(len(aft)):
        each(collect, i)
        if i == len(aft) - 1:
            out_close()
        tally(i)

    values = win_v[...].astype(F32).reshape(units, e)
    scaling = rms_scaling(values)
    unit = values * scaling
    g = dot((grad_hid[...] * slope[...]).astype(BF16), w_in_v[...], 1, 1) * egain[...].reshape(1, e)
    grad_enc = acc[...].reshape(units, e)
    out = grad_enc + scaling * (g - unit * jnp.mean(g * unit, axis=-1, keepdims=True))
    out = out.reshape(rows_dev, 2 * UNIT, e)
    keep = gdb.shape[0]
    for n in range(2):
        @pl.when(c == n)
        def _(n=n):
            at = (2 * UNIT - keep) * n
            gdb[...] = jnp.swapaxes(out[:, at:at + keep, :], 0, 1)

    def drain(n):
        for i in range(len(fore)):
            ask[n][i][2]()
            for copy in ring_copies(n, i):
                copy.wait_send()
        for i in range(len(aft)):
            returns[n][i][2]()
            for k in range(nx):
                pair_copy(n, i, k, 3 - n).wait_send()
            for copy in relays(n, i) + ends(n, i):
                copy.wait_send()
            if n == 2:
                shared(i).wait_send()

    each(drain)
    for copy in out_pair() + out_relays() + out_ends():
        copy.wait_send()


def step(dims, *args):
    n_seq, nx, nb, rows_dev, e, fore, aft = dims
    shards, rows_in, db, egain, w_in, w_out, tok, gout, dgain, w_q, w_p, w_k, w_v = args
    slot = (2, UNIT, e)
    high, width = tok.shape[0], w_q.shape[1]
    lanes = 2 * nx
    cols = tok.shape[1] // lanes
    half = nb // 2
    units = rows_dev * 2 * UNIT
    rows = nb * 3 * nx * UNIT
    nf, na = len(fore), len(aft)
    dma = pltpu.SemaphoreType.DMA
    return pl.pallas_call(
        functools.partial(step_kernel, dims),
        out_shape=(
            jax.ShapeDtypeStruct((high, cols), BF16),
            jax.ShapeDtypeStruct((high, cols), F32),
            jax.ShapeDtypeStruct((3 * UNIT // 2, rows_dev, e), F32),
        ),
        in_specs=[SM, SM, HB, VM, HB, HB, HB, HB, VM, HB, HB, HB, HB],
        out_specs=(VM, VM, VM),
        scratch_shapes=[
            pltpu.VMEM((rows_dev, *slot), BF16),
            *[pltpu.VMEM(a.shape, BF16) for a in (w_in, w_out, tok, gout, w_q, w_p, w_k, w_v)],
            pltpu.VMEM((rows_dev, *slot), BF16),
            pltpu.VMEM((units, w_in.shape[1]), F32),
            pltpu.VMEM((n_seq, *slot), BF16),
            [pltpu.VMEM((n_seq, 2, UNIT, w), BF16) for _, w in fore],
            pltpu.VMEM((nb, 3 * nx, UNIT, e), BF16),
            pltpu.VMEM((high, width), BF16),
            pltpu.VMEM((high, width), BF16),
            pltpu.VMEM((high, 1), F32),
            pltpu.VMEM((2, rows, width), F32),
            pltpu.VMEM((high, width), BF16),
            pltpu.VMEM((high, width), BF16),
            pltpu.VMEM((2, rows, width), BF16),
            pltpu.VMEM((nb, 3 * nx, UNIT, e), BF16),
            pltpu.VMEM((nx, nb, *slot), BF16),
            pltpu.VMEM((2, half, *slot), BF16),
            pltpu.VMEM((2, nb, *slot), BF16),
            pltpu.VMEM((nx, nb, *slot), BF16),
            pltpu.VMEM((nb, *slot), BF16),
            [pltpu.VMEM((n_seq, 2, UNIT, w), BF16) for _, w in aft],
            [pltpu.VMEM((n_seq, 2, UNIT, w), BF16) for _, w in aft],
            pltpu.VMEM((rows_dev, *slot), F32),
            pltpu.VMEM((units, w_in.shape[1]), F32),
            pltpu.VMEM((lanes, high, cols), F32),
            pltpu.VMEM((nx, 2, 2, high, cols), BF16),
            pltpu.VMEM((nx, 2, high, cols), BF16),
            pltpu.VMEM((2, high, cols), BF16),
            pltpu.VMEM((nx, 2, high, cols), BF16),
            pltpu.VMEM((2, 2, high, cols), BF16),
            pltpu.SMEM((n_seq,), jnp.int32),
            pltpu.SMEM((n_seq,), jnp.int32),
            pltpu.SMEM((n_seq,), jnp.int32),
            dma((9,)),
            dma((nf, n_seq)),
            dma((nf, n_seq)),
            dma((nf, 11)),
            dma((nf, 11)),
            dma((na, nx + 4)),
            dma((na, nx + 4)),
            dma((nx + 4,)),
            dma((nx + 4,)),
            dma((na, n_seq)),
            dma((na, n_seq)),
            dma((na,)),
            dma((na,)),
        ],
        compiler_params=pltpu.CompilerParams(
            collective_id=0, has_side_effects=True, vmem_limit_bytes=BIG
        ),
        name="step",
    )(*args)


def body(
    n_seq, nx,
    tokens, database, nb_shard, nb_row, dec_gain, enc_gain,
    w_in, w_out, w_query, w_key, w_value, w_proj, grad_out,
):
    rows_dev, length, e = database.shape
    nb = tokens.shape[0] // STRETCH * K
    dims = (n_seq, nx, nb, rows_dev, e, cuts(e, FORE), cuts(e, AFT))
    cca, gtok, gdb = step(
        dims, nb_shard.T, nb_row.T, database.reshape(rows_dev, length // UNIT, UNIT, e), enc_gain,
        w_in, w_out, tokens, grad_out, dec_gain.reshape(1, -1), w_query, w_proj, w_key, w_value,
    )
    return cca, gtok, jnp.swapaxes(gdb, 0, 1)


def solution(mesh):
    n_seq = mesh.shape["seq"]
    nx = mesh.shape["mp"] // 2
    split = Mesh(mesh.devices.reshape(n_seq, nx, 2), ("seq", "mp_0", "mp_1"))
    placed = (
        P("seq", None),
        P("seq", None, None),
        P(),
        P(),
        P(),
        P(),
        P(),
        P(),
        P(None, MP),
        P(None, MP),
        P(None, MP),
        P(MP, None),
        P("seq", None),
    )
    return jax.shard_map(
        functools.partial(body, n_seq, nx),
        mesh=split,
        in_specs=placed,
        out_specs=(P("seq", MP), P("seq", MP), P("seq", MP, None)),
        check_vma=False,
    )
```

```python
import functools

import jax
import jax.numpy as jnp
from jax import lax
from jax.experimental import pallas as pl
from jax.experimental.pallas import tpu as pltpu
from jax.sharding import Mesh
from jax.sharding import PartitionSpec as P

HD = 128
STRETCH = 64
K = 2
SEQ_LEN = 4096
UNIT = 8
EPSILON = 1e-06
MP = ("mp_0", "mp_1")
F32 = jnp.float32
BF16 = jnp.bfloat16
VM = pl.BlockSpec(memory_space=pltpu.VMEM)
SM = pl.BlockSpec(memory_space=pltpu.SMEM)
HB = pl.BlockSpec(memory_space=pltpu.HBM)
BIG = 46000 * 1024
FORE = (4, 2, 1)
AFT = (2, 3, 2)


def rcopy(src, dst, ssem, rsem, **where):
    return pltpu.make_async_remote_copy(
        src_ref=src,
        dst_ref=dst,
        send_sem=ssem,
        recv_sem=rsem,
        device_id=where,
        device_id_type=pl.DeviceIdType.MESH,
    )


def dot(a, b, ca=1, cb=0):
    return lax.dot_general(a, b, (((ca,), (cb,)), ((), ())), preferred_element_type=F32)


def rms_scaling(values):
    return lax.rsqrt(jnp.mean(values * values, axis=-1, keepdims=True) + EPSILON)


def sigmoid(v):
    return 1.0 / (1.0 + jnp.exp(-v))


def greet(n_seq, nx):
    me, x, c = lax.axis_index("seq"), lax.axis_index("mp_0"), lax.axis_index("mp_1")
    barrier = pltpu.get_barrier_semaphore()

    def tell(**where):
        pl.semaphore_signal(barrier, inc=1, device_id=where, device_id_type=pl.DeviceIdType.MESH)

    def far(k, carry):
        tell(seq=lax.rem(me + k, n_seq))
        return carry

    lax.fori_loop(1, n_seq, far, 0)
    tell(mp_0=lax.rem(x + 1, nx))
    tell(mp_0=lax.rem(x + nx - 1, nx))
    tell(mp_1=1 - c)
    return barrier, n_seq + 2


def seq_exchange(n_seq, n, src, dst, send, recv, src_lanes=None):
    me = lax.axis_index("seq")

    def piece(k, sending):
        peer = lax.rem(me + k, n_seq) if sending else lax.rem(me + n_seq - k, n_seq)
        at = me if sending else peer
        if src_lanes is None:
            a, b = src.at[peer, pl.ds(0, n)], dst.at[at, pl.ds(0, n)]
        else:
            a, b = src.at[peer, pl.ds(0, n), :, src_lanes], dst.at[at, pl.ds(0, n)]
        return rcopy(a, b, send.at[peer], recv.at[at], seq=peer)

    def run(sending, act):
        def go(k, carry):
            act(piece(k, sending))
            return carry

        lax.fori_loop(1, n_seq, go, 0)

    return (
        lambda: run(True, lambda copy: copy.start()),
        lambda: run(False, lambda copy: copy.wait_recv()),
        lambda: run(True, lambda copy: copy.wait_send()),
    )


def cuts(e, sizes):
    tiles = e // 128
    at, out = 0, []
    for i, share in enumerate(sizes):
        wide = tiles - at if i == len(sizes) - 1 else max(1, tiles * share // sum(sizes))
        out.append((at * 128, wide * 128))
        at += wide
    return out


def loop(count, f):
    def go(i, carry):
        f(i)
        return carry

    lax.fori_loop(0, count, go, 0)


def step_kernel(
    dims,
    shards, rows_in, db, egain, w_in, w_out, tok, gout, dgain, w_q, w_p, w_k, w_v,
    cca, gtok, gdb,
    win_v, w_in_v, w_out_v, tok_v, gout_v, w_q_v, w_p_v, w_k_v, w_v_v,
    enc, slope, outg, recvs, full, q, gctx, tscale, kv, ctx, dq, dkv,
    terms, sib, relay, last, comb, ge, back, got_back, acc, grad_hid,
    gn, outs, osib, orelay, ocomb, fin,
    rows_s, name_s, pick_s,
    lsem, a_send, a_recv, b_send, b_recv, d_send, d_recv, o_send, o_recv, e_send, e_recv, f_send, f_recv,
):
    n_seq, nx, nb, rows_dev, e, fore, aft = dims
    me, x, c = lax.axis_index("seq"), lax.axis_index("mp_0"), lax.axis_index("mp_1")
    half = nb // 2
    per_dev = nb // K
    right, left, opp = lax.rem(x + 1, nx), lax.rem(x + nx - 1, nx), lax.rem(x + 2, nx)
    branches = (1, 2)

    def each(f, *args):
        for n in branches:
            @pl.when(c == n - 1)
            def _(n=n):
                f(n, *args)

    loads = [
        pltpu.make_async_copy(s, d, lsem.at[i])
        for i, (s, d) in enumerate(
            (
                (db.at[:, pl.ds(3 * x + c, 2)], win_v),
                (w_in, w_in_v),
                (w_out, w_out_v),
                (tok, tok_v),
                (w_q, w_q_v),
                (gout, gout_v),
                (w_p, w_p_v),
                (w_k, w_k_v),
                (w_v, w_v_v),
            )
        )
    ]
    for load in loads[:3]:
        load.start()
    barrier, greeted = greet(n_seq, nx)

    def find(d):
        row, named = jnp.int32(0), jnp.int32(-1)
        for k in range(nb):
            hit = shards[k % K, d * per_dev + k // K] == me
            at = rows_in[k % K, d * per_dev + k // K]
            row, named = jnp.where(hit, at, row), jnp.where(hit, at, named)
        rows_s[d] = row
        name_s[d] = named

    loop(n_seq, find)

    units = rows_dev * 2 * UNIT
    loads[0].wait()
    values = win_v[...].astype(F32).reshape(units, e)
    gain = egain[...].reshape(1, e)
    normed = (values * rms_scaling(values) * gain).astype(BF16)
    loads[1].wait()
    pre = dot(normed, w_in_v[...])
    gate = sigmoid(pre)
    slope[...] = gate * (1.0 + pre * (1.0 - gate))
    hidden = (pre * gate).astype(BF16)
    loads[2].wait()
    for load in loads[3:]:
        load.start()
    encoded = values + dot(hidden, w_out_v[...])
    enc[...] = encoded.reshape(rows_dev, 2, UNIT, e).astype(BF16)

    def stage_out(d):
        outg[d] = enc[rows_s[d]]

    loop(n_seq, stage_out)
    for (l0, w), recv in zip(fore, recvs):
        recv[me] = outg[me, :, :, l0:l0 + w]
    pl.semaphore_wait(barrier, greeted)

    ask = {
        n: [
            seq_exchange(n_seq, n, outg, recv, a_send.at[i], a_recv.at[i], pl.ds(l0, w))
            for i, ((l0, w), recv) in enumerate(zip(fore, recvs))
        ]
        for n in branches
    }

    def ask_start(n):
        for plan in ask[n]:
            plan[0]()

    each(ask_start)

    size = min(128, q.shape[0])
    blocks = q.shape[0] // size
    loads[3].wait()
    loads[4].wait()

    def query(i):
        at = pl.ds(pl.multiple_of(i * size, size), size)
        vals = tok_v[at, :].astype(F32)
        scale = rms_scaling(vals)
        tscale[at, :] = scale
        q[at, :] = dot((vals * scale * dgain[...]).astype(BF16), w_q_v[...]).astype(BF16)

    loop(blocks, query)
    loads[5].wait()
    loads[6].wait()

    def context_grad(i):
        at = pl.ds(pl.multiple_of(i * size, size), size)
        where = me * q.shape[0] + i * size + lax.broadcasted_iota(jnp.int32, (size, 1), 0)
        alive = lax.rem(where // STRETCH, SEQ_LEN // STRETCH) != 0
        grad = dot(gout_v[at, :], w_p_v[...], 1, 1)
        gctx[at, :] = jnp.where(alive, grad, 0.0).astype(BF16)

    loop(blocks, context_grad)
    loads[7].wait()
    loads[8].wait()

    def mine(n, i, xx):
        l0, w = fore[i]
        return full.at[:, pl.ds(3 * xx + n - 1, n), :, pl.ds(l0, w)]

    def part(n, i, xx, h):
        l0, w = fore[i]
        return full.at[pl.ds(half * h, half), pl.ds(3 * xx + n - 1, n), :, pl.ds(l0, w)]

    def ring(n, i, k, ref, **where):
        return rcopy(ref, ref, b_send.at[i, k], b_recv.at[i, k], **where)

    def ring_copies(n, i):
        sib_to = dict(mp_1=1 - c)
        return [
            ring(n, i, 0, part(n, i, x, 0), mp_0=right),
            ring(n, i, 1, part(n, i, x, 1), mp_0=left),
            ring(n, i, 2, part(n, i, x, 1), mp_0=right),
            ring(n, i, 3, part(n, i, x, 0), mp_0=left),
            ring(n, i, 4, mine(n, i, x), **sib_to),
            ring(n, i, 5, part(n, i, left, 0), mp_0=right),
            ring(n, i, 6, part(n, i, right, 1), mp_0=left),
            ring(n, i, 7, mine(n, i, left), **sib_to),
            ring(n, i, 8, mine(n, i, right), **sib_to),
            ring(n, i, 9, part(n, i, opp, 0), **sib_to),
            ring(n, i, 10, part(n, i, opp, 1), **sib_to),
        ]

    def ring_got(n, i, k):
        ref = {
            0: lambda: part(n, i, left, 0),
            1: lambda: part(n, i, right, 1),
            2: lambda: part(n, i, left, 1),
            3: lambda: part(n, i, right, 0),
            4: lambda: mine(n, i, x),
            5: lambda: part(n, i, opp, 0),
            6: lambda: part(n, i, opp, 1),
            7: lambda: mine(n, i, left),
            8: lambda: mine(n, i, right),
            9: lambda: part(n, i, opp, 0),
            10: lambda: part(n, i, opp, 1),
        }[k]()
        ring(n, i, k, ref, mp_1=1 - c).wait_recv()

    def ring_open(n, i):
        ask[n][i][1]()
        l0, w = fore[i]

        def pick(j):
            slot = shards[lax.rem(j, K), me * per_dev + j // K]
            for u in range(n):
                full[j, 3 * x + n - 1 + u, :, l0:l0 + w] = recvs[i][slot, u]

        loop(nb, pick)
        for copy in ring_copies(n, i)[:5]:
            copy.start()

    def ring_pass(n, i):
        copies = ring_copies(n, i)
        ring_got(n, i, 0)
        copies[5].start()
        ring_got(n, i, 1)
        copies[6].start()
        ring_got(n, i, 2)
        copies[7].start()
        ring_got(n, i, 3)
        copies[8].start()

    def ring_close(n, i):
        copies = ring_copies(n, i)
        ring_got(n, i, 5)
        copies[9].start()
        ring_got(n, i, 6)
        copies[10].start()
        for k in (4, 7, 8, 9, 10):
            ring_got(3 - n, i, k)

    span = K * 12 * UNIT * nx // 4
    many = max(1, per_dev // 2)
    turns = per_dev // many
    tall = many * span

    def project(i):
        l0, w = fore[i]

        def go(t):
            at = pl.ds(pl.multiple_of(t * tall, tall), tall)
            rows = full[pl.ds(t * many * K, many * K), :, :, l0:l0 + w]
            rows = rows.astype(F32).reshape(tall, w).astype(BF16)
            for h, weight in enumerate((w_k_v, w_v_v)):
                out = dot(rows, weight[l0:l0 + w, :])
                if i:
                    out = out + kv[h, at, :]
                kv[h, at, :] = out

        loop(turns, go)

    each(ring_open, 0)
    for i in range(1, len(fore)):
        each(ring_pass, i - 1)
        each(ring_open, i)
        each(ring_close, i - 1)
        project(i - 1)
    each(ring_pass, len(fore) - 1)
    each(ring_close, len(fore) - 1)
    project(len(fore) - 1)

    width = q.shape[1]
    heads = width // HD
    factor = HD ** (-0.5)

    def attend(t):
        at = pl.ds(pl.multiple_of(t * tall, tall), tall)
        here = pl.ds(pl.multiple_of(t * many * STRETCH, many * STRETCH), many * STRETCH)
        todo = [(s, h) for s in range(many) for h in range(heads)]

        def pieces(block, high):
            return {
                (s, h): block[s * high:(s + 1) * high, h * HD:(h + 1) * HD] for s, h in todo
            }

        qs, gs = pieces(q[here, :], STRETCH), pieces(gctx[here, :], STRETCH)
        ks, vs = pieces(kv[0, at, :].astype(BF16), span), pieces(kv[1, at, :].astype(BF16), span)
        exps = {p: jnp.exp(dot(qs[p], ks[p], 1, 1) * factor) for p in todo}
        dps = {p: dot(gs[p], vs[p], 1, 1) for p in todo}
        probs = {p: exps[p] / jnp.sum(exps[p], axis=-1, keepdims=True) for p in todo}
        weights = {p: probs[p].astype(BF16) for p in todo}
        scores = {
            p: (
                probs[p] * (dps[p] - jnp.sum(probs[p] * dps[p], axis=-1, keepdims=True)) * factor
            ).astype(BF16)
            for p in todo
        }
        for s in range(many):
            lines = pl.ds(pl.multiple_of((t * many + s) * STRETCH, STRETCH), STRETCH)
            ends = pl.ds(pl.multiple_of((t * many + s) * span, span), span)
            for h in range(heads):
                p, lanes = (s, h), slice(h * HD, (h + 1) * HD)
                ctx[lines, lanes] = dot(weights[p], vs[p]).astype(BF16)
                dq[lines, lanes] = dot(scores[p], ks[p]).astype(BF16)
                dkv[0, ends, lanes] = dot(scores[p], qs[p], 0, 0).astype(BF16)
                dkv[1, ends, lanes] = dot(weights[p], gs[p], 0, 0).astype(BF16)

    loop(turns, attend)

    def lanes_of(i):
        l0, w = aft[i]
        return pl.ds(l0, w)

    def pair_copy(n, i, k, m):
        return rcopy(
            terms.at[:, pl.ds(3 * k + m - 1, m), :, lanes_of(i)],
            sib.at[k, :, pl.ds(0, m), :, lanes_of(i)],
            d_send.at[i, k],
            d_recv.at[i, k],
            mp_1=1 - c,
        )

    def pair_start(n, i):
        for k in (opp, left, right, x):
            pair_copy(n, i, k, 3 - n).start()

    toward = (right, left)

    def piece(n, i, k, h, to, dst, sem):
        return rcopy(
            comb.at[k, pl.ds(half * h, half), pl.ds(0, n), :, lanes_of(i)],
            dst.at[:, pl.ds(0, n), :, lanes_of(i)],
            d_send.at[i, sem],
            d_recv.at[i, sem],
            mp_0=to,
        )

    def relay_of(n, i, h):
        return piece(n, i, opp, h, toward[h], relay.at[h], nx + h)

    def plain_of(n, i, h):
        to = toward[1 - h]
        return piece(n, i, to, h, to, last.at[1 - h, pl.ds(half * h, half)], nx + 2 + h)

    def final_of(n, i, h):
        to = toward[h]
        return piece(n, i, to, h, to, last.at[h, pl.ds(half * h, half)], nx + 4 + h)

    def reduce_pair(n, i):
        l0, w = aft[i]

        def add(k):
            pair_copy(n, i, k, n).wait_recv()

            def go(j):
                for u in range(n):
                    comb[k, j, u, :, l0:l0 + w] = (
                        terms[j, 3 * k + n - 1 + u, :, l0:l0 + w].astype(F32)
                        + sib[k, j, u, :, l0:l0 + w].astype(F32)
                    ).astype(BF16)

            loop(nb, go)

        add(opp)
        for h in range(2):
            relay_of(n, i, h).start()
        for h in range(2):
            add(toward[1 - h])
            plain_of(n, i, h).start()
        add(x)

    def reduce_ends(n, i):
        l0, w = aft[i]
        for h in range(2):
            relay_of(n, i, h).wait_recv()

            def add(j, h=h):
                for u in range(n):
                    comb[toward[h], half * h + j, u, :, l0:l0 + w] = (
                        comb[toward[h], half * h + j, u, :, l0:l0 + w].astype(F32)
                        + relay[h, j, u, :, l0:l0 + w].astype(F32)
                    ).astype(BF16)

            loop(half, add)
            final_of(n, i, h).start()

    def give_back(n, i):
        l0, w = aft[i]
        for h in range(2):
            plain_of(n, i, h).wait_recv()
            final_of(n, i, h).wait_recv()

        def add(j):
            for u in range(n):
                ge[j, u, :, l0:l0 + w] = (
                    comb[x, j, u, :, l0:l0 + w].astype(F32)
                    + last[0, j, u, :, l0:l0 + w].astype(F32)
                    + last[1, j, u, :, l0:l0 + w].astype(F32)
                ).astype(BF16)

        loop(nb, add)

        def stage(s):
            spot = pick_s[s]
            for u in range(n):
                back[i][s, u] = ge[spot, u, :, l0:l0 + w]

        loop(n_seq, stage)
        for u in range(n):
            got_back[i][me, u] = back[i][me, u]
        returns[n][i][0]()

    returns = {
        n: [
            seq_exchange(n_seq, n, back[i], got_back[i], e_send.at[i], e_recv.at[i])
            for i in range(len(aft))
        ]
        for n in branches
    }

    def shared(i):
        return rcopy(
            got_back[i].at[:, 0], got_back[i].at[:, 1], f_send.at[i], f_recv.at[i], mp_1=1 - c
        )

    def terms_of(i):
        l0, w = aft[i]

        def go(t):
            at = pl.ds(pl.multiple_of(t * tall, tall), tall)
            out = dot(dkv[0, at, :], w_k_v[l0:l0 + w, :], 1, 1)
            out = out + dot(dkv[1, at, :], w_v_v[l0:l0 + w, :], 1, 1)
            terms[pl.ds(t * many * K, many * K), :, :, l0:l0 + w] = out.reshape(
                many * K, 3 * nx, UNIT, w
            ).astype(BF16)

        loop(turns, go)

    def find_back(s):
        spot = jnp.int32(0)
        for k in range(nb):
            spot = jnp.where(shards[k % K, me * per_dev + k // K] == s, k, spot)
        pick_s[s] = spot

    high = ctx.shape[0]
    lanes = 2 * nx
    cols = tok_v.shape[1] // lanes
    live = lax.rem(
        (me * high + lax.broadcasted_iota(jnp.int32, (high, 1), 0)) // STRETCH, SEQ_LEN // STRETCH
    ) != 0

    def columns(l):
        return pl.ds(pl.multiple_of(l * cols, cols), cols)

    def out_terms():
        def forward(l):
            out = dot(ctx[...], w_p_v[:, columns(l)])
            outs[l // 2, lax.rem(l, 2), 0] = jnp.where(live, out, 0.0).astype(BF16)

        loop(lanes, forward)

    def grad_terms():
        def backward(l, total):
            grad = dot(dq[...], w_q_v[columns(l), :], 1, 1) * dgain[:, columns(l)]
            gn[l] = grad
            return total + jnp.sum(
                grad * tok_v[:, columns(l)].astype(F32), axis=-1, keepdims=True
            )

        total = lax.fori_loop(0, lanes, backward, jnp.zeros((high, 1), F32))
        scale = tscale[...]
        tilt = total * scale * scale / (lanes * cols)

        def finish(l):
            grad = scale * (gn[l] - tok_v[:, columns(l)].astype(F32) * tilt)
            outs[l // 2, lax.rem(l, 2), 1] = grad.astype(BF16)

        loop(lanes, finish)

    def out_pair(k, h):
        return rcopy(
            outs.at[k, 1 - c, h], osib.at[k, h], o_send.at[h, k], o_recv.at[h, k], mp_1=1 - c
        )

    def out_piece(k, h, to, dst, sem):
        return rcopy(ocomb.at[k, h], dst, o_send.at[h, sem], o_recv.at[h, sem], mp_0=to)

    def out_relay(h):
        return out_piece(opp, h, toward[h], orelay.at[h], nx)

    def out_plain(h):
        to = toward[1 - h]
        return out_piece(to, h, to, fin.at[1 - h, h], nx + 1)

    def out_final(h):
        to = toward[h]
        return out_piece(to, h, to, fin.at[h, h], nx + 2)

    def out_open(h):
        for k in (opp, left, right, x):
            out_pair(k, h).start()

    def by_stretch(f):
        loop(high // STRETCH, lambda i: f(pl.ds(pl.multiple_of(i * STRETCH, STRETCH), STRETCH)))

    def out_reduce_pair(h):
        def add(k):
            out_pair(k, h).wait_recv()

            def go(at):
                ocomb[k, h, at, :] = (
                    outs[k, c, h, at, :].astype(F32) + osib[k, h, at, :].astype(F32)
                ).astype(BF16)

            by_stretch(go)

        add(opp)
        out_relay(h).start()
        add(toward[1 - h])
        out_plain(h).start()
        add(toward[h])
        add(x)

    def out_reduce_ends(h):
        out_relay(h).wait_recv()

        def go(at):
            ocomb[toward[h], h, at, :] = (
                ocomb[toward[h], h, at, :].astype(F32) + orelay[h, at, :].astype(F32)
            ).astype(BF16)

        by_stretch(go)
        out_final(h).start()

    def out_close(h, target):
        out_plain(h).wait_recv()
        out_final(h).wait_recv()

        def go(at):
            total = ocomb[x, h, at, :].astype(F32) + fin[0, h, at, :].astype(F32)
            target[at, :] = (total + fin[1, h, at, :].astype(F32)).astype(target.dtype)

        by_stretch(go)

    m = len(aft)
    for i in range(m):
        terms_of(i)
        each(pair_start, i)
    loop(n_seq, find_back)
    out_terms()
    out_open(0)
    each(reduce_pair, 0)
    each(reduce_pair, 1)
    grad_terms()
    out_open(1)
    each(reduce_ends, 0)
    for i in range(2, m):
        each(reduce_pair, i)
    out_reduce_pair(0)
    each(reduce_ends, 1)
    each(give_back, 0)
    for i in range(2, m):
        each(reduce_ends, i)
    out_reduce_pair(1)
    each(give_back, 1)
    out_reduce_ends(0)
    for i in range(2, m):
        each(give_back, i)
    out_reduce_ends(1)

    def collect(n, i):
        returns[n][i][1]()
        if n == 2:
            shared(i).start()
        else:
            shared(i).wait_recv()

    def tally(i):
        l0, w = aft[i]
        for u in range(2):
            def add(d, sums):
                named = name_s[d]
                slot = got_back[i][d, u].astype(F32)
                return tuple(
                    total + jnp.where(named == r, slot, 0.0) for r, total in enumerate(sums)
                )

            sums = lax.fori_loop(
                0, n_seq, add, tuple(jnp.zeros((UNIT, w), F32) for _ in range(rows_dev))
            )
            for r in range(rows_dev):
                acc[r, u, :, l0:l0 + w] = sums[r]
        part = acc[:, :, :, l0:l0 + w].reshape(units, w).astype(BF16)
        out = dot(part, w_out_v[:, l0:l0 + w], 1, 1)
        grad_hid[...] = out if i == 0 else grad_hid[...] + out

    for i in range(len(aft)):
        each(collect, i)
        tally(i)
        if i == m - 2:
            out_close(0, cca)
            out_close(1, gtok)

    values = win_v[...].astype(F32).reshape(units, e)
    scaling = rms_scaling(values)
    unit = values * scaling
    g = dot((grad_hid[...] * slope[...]).astype(BF16), w_in_v[...], 1, 1) * egain[...].reshape(1, e)
    grad_enc = acc[...].reshape(units, e)
    out = grad_enc + scaling * (g - unit * jnp.mean(g * unit, axis=-1, keepdims=True))
    out = out.reshape(rows_dev, 2 * UNIT, e)
    keep = gdb.shape[0]
    for n in range(2):
        @pl.when(c == n)
        def _(n=n):
            at = (2 * UNIT - keep) * n
            gdb[...] = jnp.swapaxes(out[:, at:at + keep, :], 0, 1)

    def drain(n):
        for i in range(len(fore)):
            ask[n][i][2]()
            for copy in ring_copies(n, i):
                copy.wait_send()
        for i in range(len(aft)):
            returns[n][i][2]()
            for k in range(nx):
                pair_copy(n, i, k, 3 - n).wait_send()
            for h in range(2):
                for copy in (relay_of(n, i, h), plain_of(n, i, h), final_of(n, i, h)):
                    copy.wait_send()
            if n == 2:
                shared(i).wait_send()

    each(drain)
    for h in range(2):
        for copy in [out_pair(k, h) for k in range(nx)] + [out_relay(h), out_plain(h), out_final(h)]:
            copy.wait_send()


def step(dims, *args):
    n_seq, nx, nb, rows_dev, e, fore, aft = dims
    shards, rows_in, db, egain, w_in, w_out, tok, gout, dgain, w_q, w_p, w_k, w_v = args
    slot = (2, UNIT, e)
    high, width = tok.shape[0], w_q.shape[1]
    lanes = 2 * nx
    cols = tok.shape[1] // lanes
    half = nb // 2
    units = rows_dev * 2 * UNIT
    rows = nb * 3 * nx * UNIT
    nf, na = len(fore), len(aft)
    dma = pltpu.SemaphoreType.DMA
    return pl.pallas_call(
        functools.partial(step_kernel, dims),
        out_shape=(
            jax.ShapeDtypeStruct((high, cols), BF16),
            jax.ShapeDtypeStruct((high, cols), F32),
            jax.ShapeDtypeStruct((3 * UNIT // 2, rows_dev, e), F32),
        ),
        in_specs=[SM, SM, HB, VM, HB, HB, HB, HB, VM, HB, HB, HB, HB],
        out_specs=(VM, VM, VM),
        scratch_shapes=[
            pltpu.VMEM((rows_dev, *slot), BF16),
            *[pltpu.VMEM(a.shape, BF16) for a in (w_in, w_out, tok, gout, w_q, w_p, w_k, w_v)],
            pltpu.VMEM((rows_dev, *slot), BF16),
            pltpu.VMEM((units, w_in.shape[1]), F32),
            pltpu.VMEM((n_seq, *slot), BF16),
            [pltpu.VMEM((n_seq, 2, UNIT, w), BF16) for _, w in fore],
            pltpu.VMEM((nb, 3 * nx, UNIT, e), BF16),
            pltpu.VMEM((high, width), BF16),
            pltpu.VMEM((high, width), BF16),
            pltpu.VMEM((high, 1), F32),
            pltpu.VMEM((2, rows, width), F32),
            pltpu.VMEM((high, width), BF16),
            pltpu.VMEM((high, width), BF16),
            pltpu.VMEM((2, rows, width), BF16),
            pltpu.VMEM((nb, 3 * nx, UNIT, e), BF16),
            pltpu.VMEM((nx, nb, *slot), BF16),
            pltpu.VMEM((2, half, *slot), BF16),
            pltpu.VMEM((2, nb, *slot), BF16),
            pltpu.VMEM((nx, nb, *slot), BF16),
            pltpu.VMEM((nb, *slot), BF16),
            [pltpu.VMEM((n_seq, 2, UNIT, w), BF16) for _, w in aft],
            [pltpu.VMEM((n_seq, 2, UNIT, w), BF16) for _, w in aft],
            pltpu.VMEM((rows_dev, *slot), F32),
            pltpu.VMEM((units, w_in.shape[1]), F32),
            pltpu.VMEM((lanes, high, cols), F32),
            pltpu.VMEM((nx, 2, 2, high, cols), BF16),
            pltpu.VMEM((nx, 2, high, cols), BF16),
            pltpu.VMEM((2, high, cols), BF16),
            pltpu.VMEM((nx, 2, high, cols), BF16),
            pltpu.VMEM((2, 2, high, cols), BF16),
            pltpu.SMEM((n_seq,), jnp.int32),
            pltpu.SMEM((n_seq,), jnp.int32),
            pltpu.SMEM((n_seq,), jnp.int32),
            dma((9,)),
            dma((nf, n_seq)),
            dma((nf, n_seq)),
            dma((nf, 11)),
            dma((nf, 11)),
            dma((na, nx + 6)),
            dma((na, nx + 6)),
            dma((2, nx + 3)),
            dma((2, nx + 3)),
            dma((na, n_seq)),
            dma((na, n_seq)),
            dma((na,)),
            dma((na,)),
        ],
        compiler_params=pltpu.CompilerParams(
            collective_id=0, has_side_effects=True, vmem_limit_bytes=BIG
        ),
        name="step",
    )(*[pltpu.with_memory_space_constraint(a, pltpu.HBM) for a in args])


def body(
    n_seq, nx,
    tokens, database, nb_shard, nb_row, dec_gain, enc_gain,
    w_in, w_out, w_query, w_key, w_value, w_proj, grad_out,
):
    rows_dev, length, e = database.shape
    nb = tokens.shape[0] // STRETCH * K
    dims = (n_seq, nx, nb, rows_dev, e, cuts(e, FORE), cuts(e, AFT))
    cca, gtok, gdb = step(
        dims, nb_shard.T, nb_row.T, database.reshape(rows_dev, length // UNIT, UNIT, e), enc_gain,
        w_in, w_out, tokens, grad_out, dec_gain.reshape(1, -1), w_query, w_proj, w_key, w_value,
    )
    return cca, gtok, jnp.swapaxes(gdb, 0, 1)


def solution(mesh):
    n_seq = mesh.shape["seq"]
    nx = mesh.shape["mp"] // 2
    split = Mesh(mesh.devices.reshape(n_seq, nx, 2), ("seq", "mp_0", "mp_1"))
    placed = (
        P("seq", None),
        P("seq", None, None),
        P(),
        P(),
        P(),
        P(),
        P(),
        P(),
        P(None, MP),
        P(None, MP),
        P(None, MP),
        P(MP, None),
        P("seq", None),
    )
    return jax.shard_map(
        functools.partial(body, n_seq, nx),
        mesh=split,
        in_specs=placed,
        out_specs=(P("seq", MP), P("seq", MP), P("seq", MP, None)),
        check_vma=False,
    )
```

```python
import functools

import jax
import jax.numpy as jnp
from jax import lax
from jax.experimental import pallas as pl
from jax.experimental.pallas import tpu as pltpu
from jax.sharding import Mesh
from jax.sharding import PartitionSpec as P

HD = 128
STRETCH = 64
K = 2
SEQ_LEN = 4096
UNIT = 8
EPSILON = 1e-06
MP = ("mp_0", "mp_1")
F32 = jnp.float32
BF16 = jnp.bfloat16
VM = pl.BlockSpec(memory_space=pltpu.VMEM)
SM = pl.BlockSpec(memory_space=pltpu.SMEM)
HB = pl.BlockSpec(memory_space=pltpu.HBM)
BIG = 46000 * 1024
FORE = (4, 3)
AFT = (3, 4)


def rcopy(src, dst, ssem, rsem, **where):
    return pltpu.make_async_remote_copy(
        src_ref=src,
        dst_ref=dst,
        send_sem=ssem,
        recv_sem=rsem,
        device_id=where,
        device_id_type=pl.DeviceIdType.MESH,
    )


def dot(a, b, ca=1, cb=0):
    return lax.dot_general(a, b, (((ca,), (cb,)), ((), ())), preferred_element_type=F32)


def rms_scaling(values):
    return lax.rsqrt(jnp.mean(values * values, axis=-1, keepdims=True) + EPSILON)


def sigmoid(v):
    return 1.0 / (1.0 + jnp.exp(-v))


def greet(n_seq, nx):
    me, x, c = lax.axis_index("seq"), lax.axis_index("mp_0"), lax.axis_index("mp_1")
    barrier = pltpu.get_barrier_semaphore()

    def tell(**where):
        pl.semaphore_signal(barrier, inc=1, device_id=where, device_id_type=pl.DeviceIdType.MESH)

    def far(k, carry):
        tell(seq=lax.rem(me + k, n_seq))
        return carry

    lax.fori_loop(1, n_seq, far, 0)
    tell(mp_0=lax.rem(x + 1, nx))
    tell(mp_0=lax.rem(x + nx - 1, nx))
    tell(mp_1=1 - c)
    return barrier, n_seq + 2


def seq_exchange(n_seq, n, src, dst, send, recv, src_lanes=None):
    me = lax.axis_index("seq")

    def copy(at, to, count, peer):
        a = src.at[pl.ds(at, count), pl.ds(0, n)]
        if src_lanes is not None:
            a = src.at[pl.ds(at, count), pl.ds(0, n), :, src_lanes]
        return rcopy(a, dst.at[pl.ds(to, count), pl.ds(0, n)], send, recv, seq=peer)

    def start():
        def go(k, carry):
            peer = lax.rem(me + k, n_seq)
            copy(peer, me, 1, peer).start()
            return carry

        lax.fori_loop(1, n_seq, go, 0)

    def whole():
        return copy(0, 0, n_seq - 1, lax.rem(me + 1, n_seq))

    return start, lambda: whole().wait_recv(), lambda: whole().wait_send()


def cuts(e, sizes):
    tiles = e // 128
    at, out = 0, []
    for i, share in enumerate(sizes):
        wide = tiles - at if i == len(sizes) - 1 else max(1, tiles * share // sum(sizes))
        out.append((at * 128, wide * 128))
        at += wide
    return out


def loop(count, f, unroll=1):
    def go(i, carry):
        f(i)
        return carry

    lax.fori_loop(0, count, go, 0, unroll=unroll)


def total_of(*parts):
    out = parts[0].astype(F32)
    for part in parts[1:]:
        out = out + part.astype(F32)
    return out.astype(BF16)


def step_kernel(
    dims,
    shards, rows_in, db, egain, w_in, w_out, tok, gout, dgain, w_q, w_p, w_k, w_v,
    cca, gtok, gdb,
    win_v, w_in_v, w_out_v, tok_v, gout_v, w_q_v, w_p_v, w_k_v, w_v_v,
    enc, slope, outg, recvs, full, q, gctx, tscale, kv, ctx, dq, dkv,
    terms, sib, relay, last, comb, ge, back, got_back, acc, grad_hid,
    gn, outs, osib, orelay, ocomb, fin,
    rows_s, name_s, pick_s,
    lsem, a_send, a_recv, b_send, b_recv, d_send, d_recv, o_send, o_recv, e_send, e_recv, f_send, f_recv,
):
    n_seq, nx, nb, rows_dev, e, fore, aft = dims
    me, x, c = lax.axis_index("seq"), lax.axis_index("mp_0"), lax.axis_index("mp_1")
    half = nb // 2
    per_dev = nb // K
    right, left, opp = lax.rem(x + 1, nx), lax.rem(x + nx - 1, nx), lax.rem(x + 2, nx)
    branches = (1, 2)

    def each(f, *args):
        for n in branches:
            @pl.when(c == n - 1)
            def _(n=n):
                f(n, *args)

    loads = [
        pltpu.make_async_copy(s, d, lsem.at[i])
        for i, (s, d) in enumerate(
            (
                (db.at[:, pl.ds(3 * x + c, 2)], win_v),
                (w_in, w_in_v),
                (w_out, w_out_v),
                (tok, tok_v),
                (w_q, w_q_v),
                (gout, gout_v),
                (w_p, w_p_v),
                (w_k, w_k_v),
                (w_v, w_v_v),
            )
        )
    ]
    for load in loads[:3]:
        load.start()
    barrier, greeted = greet(n_seq, nx)

    def find(d):
        row, named = jnp.int32(0), jnp.int32(-1)
        for k in range(nb):
            hit = shards[k % K, d * per_dev + k // K] == me
            at = rows_in[k % K, d * per_dev + k // K]
            row, named = jnp.where(hit, at, row), jnp.where(hit, at, named)
        rows_s[d] = row
        name_s[d] = named

    loop(n_seq, find, 2)

    units = rows_dev * 2 * UNIT
    loads[0].wait()
    values = win_v[...].astype(F32).reshape(units, e)
    gain = egain[...].reshape(1, e)
    normed = (values * rms_scaling(values) * gain).astype(BF16)
    loads[1].wait()
    pre = dot(normed, w_in_v[...])
    gate = sigmoid(pre)
    slope[...] = gate * (1.0 + pre * (1.0 - gate))
    hidden = (pre * gate).astype(BF16)
    loads[2].wait()
    for load in loads[3:]:
        load.start()
    encoded = values + dot(hidden, w_out_v[...])
    enc[...] = encoded.reshape(rows_dev, 2, UNIT, e).astype(BF16)

    def stage_out(d):
        outg[d] = enc[rows_s[d]]

    loop(n_seq, stage_out, 4)
    for (l0, w), recv in zip(fore, recvs):
        recv[me] = outg[me, :, :, l0:l0 + w]
    pl.semaphore_wait(barrier, greeted)

    ask = {
        n: [
            seq_exchange(n_seq, n, outg, recv, a_send.at[i], a_recv.at[i], pl.ds(l0, w))
            for i, ((l0, w), recv) in enumerate(zip(fore, recvs))
        ]
        for n in branches
    }

    def ask_start(n):
        for plan in ask[n]:
            plan[0]()

    each(ask_start)

    size = min(128, q.shape[0])
    blocks = q.shape[0] // size
    loads[3].wait()
    loads[4].wait()

    def query(i):
        at = pl.ds(pl.multiple_of(i * size, size), size)
        vals = tok_v[at, :].astype(F32)
        scale = rms_scaling(vals)
        tscale[at, :] = scale
        q[at, :] = dot((vals * scale * dgain[...]).astype(BF16), w_q_v[...]).astype(BF16)

    loop(blocks, query)
    loads[5].wait()
    loads[6].wait()

    def context_grad(i):
        at = pl.ds(pl.multiple_of(i * size, size), size)
        where = me * q.shape[0] + i * size + lax.broadcasted_iota(jnp.int32, (size, 1), 0)
        alive = lax.rem(where // STRETCH, SEQ_LEN // STRETCH) != 0
        grad = dot(gout_v[at, :], w_p_v[...], 1, 1)
        gctx[at, :] = jnp.where(alive, grad, 0.0).astype(BF16)

    loop(blocks, context_grad)
    loads[7].wait()
    loads[8].wait()

    def mine(n, i, xx):
        l0, w = fore[i]
        return full.at[:, pl.ds(3 * xx + n - 1, n), :, pl.ds(l0, w)]

    def part(n, i, xx, h):
        l0, w = fore[i]
        return full.at[pl.ds(half * h, half), pl.ds(3 * xx + n - 1, n), :, pl.ds(l0, w)]

    def ring(n, i, k, ref, **where):
        return rcopy(ref, ref, b_send.at[i, k], b_recv.at[i, k], **where)

    def ring_copies(n, i):
        sib_to = dict(mp_1=1 - c)
        return [
            ring(n, i, 0, part(n, i, x, 0), mp_0=right),
            ring(n, i, 1, part(n, i, x, 1), mp_0=left),
            ring(n, i, 2, part(n, i, x, 1), mp_0=right),
            ring(n, i, 3, part(n, i, x, 0), mp_0=left),
            ring(n, i, 4, mine(n, i, x), **sib_to),
            ring(n, i, 5, part(n, i, left, 0), mp_0=right),
            ring(n, i, 6, part(n, i, right, 1), mp_0=left),
            ring(n, i, 7, mine(n, i, left), **sib_to),
            ring(n, i, 8, mine(n, i, right), **sib_to),
            ring(n, i, 9, part(n, i, opp, 0), **sib_to),
            ring(n, i, 10, part(n, i, opp, 1), **sib_to),
        ]

    def ring_got(n, i, k):
        ref = {
            0: lambda: part(n, i, left, 0),
            1: lambda: part(n, i, right, 1),
            2: lambda: part(n, i, left, 1),
            3: lambda: part(n, i, right, 0),
            4: lambda: mine(n, i, x),
            5: lambda: part(n, i, opp, 0),
            6: lambda: part(n, i, opp, 1),
            7: lambda: mine(n, i, left),
            8: lambda: mine(n, i, right),
            9: lambda: part(n, i, opp, 0),
            10: lambda: part(n, i, opp, 1),
        }[k]()
        ring(n, i, k, ref, mp_1=1 - c).wait_recv()

    def ring_open(n, i):
        ask[n][i][1]()
        l0, w = fore[i]

        for j in range(nb):
            slot = shards[j % K, me * per_dev + j // K]
            for u in range(n):
                full[j, 3 * x + n - 1 + u, :, l0:l0 + w] = recvs[i][slot, u]
        for copy in ring_copies(n, i)[:5]:
            copy.start()

    def ring_pass(n, i):
        copies = ring_copies(n, i)
        ring_got(n, i, 0)
        copies[5].start()
        ring_got(n, i, 1)
        copies[6].start()

    def ring_share(n, i):
        copies = ring_copies(n, i)
        ring_got(n, i, 2)
        copies[7].start()
        ring_got(n, i, 3)
        copies[8].start()

    def ring_close(n, i):
        copies = ring_copies(n, i)
        ring_got(n, i, 5)
        copies[9].start()
        ring_got(n, i, 6)
        copies[10].start()
        for k in (4, 7, 8, 9, 10):
            ring_got(3 - n, i, k)

    span = K * 12 * UNIT * nx // 4
    many = max(1, per_dev // 2)
    turns = per_dev // many
    tall = many * span

    def project(i):
        l0, w = fore[i]

        def go(t):
            at = pl.ds(pl.multiple_of(t * tall, tall), tall)
            rows = full[pl.ds(t * many * K, many * K), :, :, l0:l0 + w]
            rows = rows.astype(F32).reshape(tall, w).astype(BF16)
            for h, weight in enumerate((w_k_v, w_v_v)):
                out = dot(rows, weight[l0:l0 + w, :])
                if i:
                    out = out + kv[h, at, :]
                kv[h, at, :] = out

        loop(turns, go)

    each(ring_open, 0)
    each(ring_pass, 0)
    for i in range(1, len(fore)):
        each(ring_open, i)
        each(ring_share, i - 1)
        each(ring_pass, i)
        each(ring_close, i - 1)
        project(i - 1)
    each(ring_share, len(fore) - 1)
    each(ring_close, len(fore) - 1)
    project(len(fore) - 1)

    width = q.shape[1]
    heads = width // HD
    factor = HD ** (-0.5)

    def attend(t):
        at = pl.ds(pl.multiple_of(t * tall, tall), tall)
        here = pl.ds(pl.multiple_of(t * many * STRETCH, many * STRETCH), many * STRETCH)
        todo = [(s, h) for s in range(many) for h in range(heads)]

        def pieces(block, high):
            return {
                (s, h): block[s * high:(s + 1) * high, h * HD:(h + 1) * HD] for s, h in todo
            }

        qs, gs = pieces(q[here, :], STRETCH), pieces(gctx[here, :], STRETCH)
        ks, vs = pieces(kv[0, at, :].astype(BF16), span), pieces(kv[1, at, :].astype(BF16), span)
        exps = {p: jnp.exp(dot(qs[p], ks[p], 1, 1) * factor) for p in todo}
        dps = {p: dot(gs[p], vs[p], 1, 1) for p in todo}
        probs = {p: exps[p] / jnp.sum(exps[p], axis=-1, keepdims=True) for p in todo}
        weights = {p: probs[p].astype(BF16) for p in todo}
        scores = {
            p: (
                probs[p] * (dps[p] - jnp.sum(probs[p] * dps[p], axis=-1, keepdims=True)) * factor
            ).astype(BF16)
            for p in todo
        }
        for s in range(many):
            lines = pl.ds(pl.multiple_of((t * many + s) * STRETCH, STRETCH), STRETCH)
            ends = pl.ds(pl.multiple_of((t * many + s) * span, span), span)
            for h in range(heads):
                p, lanes = (s, h), slice(h * HD, (h + 1) * HD)
                ctx[lines, lanes] = dot(weights[p], vs[p]).astype(BF16)
                dq[lines, lanes] = dot(scores[p], ks[p]).astype(BF16)
                dkv[0, ends, lanes] = dot(scores[p], qs[p], 0, 0).astype(BF16)
                dkv[1, ends, lanes] = dot(weights[p], gs[p], 0, 0).astype(BF16)

    loop(turns, attend)

    def lanes_of(i):
        l0, w = aft[i]
        return pl.ds(l0, w)

    def pair_copy(n, i, k, m):
        return rcopy(
            terms.at[:, pl.ds(3 * k + m - 1, m), :, lanes_of(i)],
            sib.at[k, :, pl.ds(0, m), :, lanes_of(i)],
            d_send.at[i, k],
            d_recv.at[i, k],
            mp_1=1 - c,
        )

    def pair_start(n, i):
        for k in (opp, left, right, x):
            pair_copy(n, i, k, 3 - n).start()

    toward = (right, left)

    def piece(n, i, k, h, to, dst, sem):
        return rcopy(
            comb.at[k, pl.ds(half * h, half), pl.ds(0, n), :, lanes_of(i)],
            dst.at[:, pl.ds(0, n), :, lanes_of(i)],
            d_send.at[i, sem],
            d_recv.at[i, sem],
            mp_0=to,
        )

    def relay_of(n, i, h):
        return piece(n, i, opp, h, toward[h], relay.at[h], nx + h)

    def plain_of(n, i, h):
        to = toward[1 - h]
        return piece(n, i, to, h, to, last.at[1 - h, pl.ds(half * h, half)], nx + 2 + h)

    def final_of(n, i, h):
        to = toward[h]
        return piece(n, i, to, h, to, last.at[h, pl.ds(half * h, half)], nx + 4 + h)

    def reduce_pair(n, i):
        l0, w = aft[i]

        def add(k):
            pair_copy(n, i, k, n).wait_recv()
            comb[k, :, 0:n, :, l0:l0 + w] = total_of(
                terms[:, pl.ds(3 * k + n - 1, n), :, l0:l0 + w], sib[k, :, 0:n, :, l0:l0 + w]
            )

        add(opp)
        for h in range(2):
            relay_of(n, i, h).start()
        for h in range(2):
            add(toward[1 - h])
            plain_of(n, i, h).start()
        add(x)

    def reduce_ends(n, i):
        l0, w = aft[i]
        for h in range(2):
            relay_of(n, i, h).wait_recv()
            at = (toward[h], slice(half * h, half * h + half), slice(0, n), slice(None), slice(l0, l0 + w))
            comb[at] = total_of(comb[at], relay[h, :, 0:n, :, l0:l0 + w])
            final_of(n, i, h).start()

    def give_back(n, i):
        l0, w = aft[i]
        for h in range(2):
            plain_of(n, i, h).wait_recv()
            final_of(n, i, h).wait_recv()

        at = (slice(None), slice(0, n), slice(None), slice(l0, l0 + w))
        ge[at] = total_of(comb[(x, *at)], last[(0, *at)], last[(1, *at)])

        def stage(s):
            spot = pick_s[s]
            for u in range(n):
                back[i][s, u] = ge[spot, u, :, l0:l0 + w]

        loop(n_seq, stage, 8)
        for u in range(n):
            got_back[i][me, u] = back[i][me, u]
        returns[n][i][0]()

    returns = {
        n: [
            seq_exchange(n_seq, n, back[i], got_back[i], e_send.at[i], e_recv.at[i])
            for i in range(len(aft))
        ]
        for n in branches
    }

    def shared(i):
        return rcopy(
            got_back[i].at[:, 0], got_back[i].at[:, 1], f_send.at[i], f_recv.at[i], mp_1=1 - c
        )

    def terms_of(i):
        l0, w = aft[i]

        def go(t):
            at = pl.ds(pl.multiple_of(t * tall, tall), tall)
            out = dot(dkv[0, at, :], w_k_v[l0:l0 + w, :], 1, 1)
            out = out + dot(dkv[1, at, :], w_v_v[l0:l0 + w, :], 1, 1)
            terms[pl.ds(t * many * K, many * K), :, :, l0:l0 + w] = out.reshape(
                many * K, 3 * nx, UNIT, w
            ).astype(BF16)

        loop(turns, go)

    def find_back(s):
        spot = jnp.int32(0)
        for k in range(nb):
            spot = jnp.where(shards[k % K, me * per_dev + k // K] == s, k, spot)
        pick_s[s] = spot

    high = ctx.shape[0]
    lanes = 2 * nx
    cols = tok_v.shape[1] // lanes
    live = lax.rem(
        (me * high + lax.broadcasted_iota(jnp.int32, (high, 1), 0)) // STRETCH, SEQ_LEN // STRETCH
    ) != 0

    def columns(l):
        return pl.ds(pl.multiple_of(l * cols, cols), cols)

    def out_terms():
        def forward(l):
            out = dot(ctx[...], w_p_v[:, columns(l)])
            outs[l // 2, lax.rem(l, 2), 0] = jnp.where(live, out, 0.0).astype(BF16)

        loop(lanes, forward)

    def grad_terms():
        def backward(l, total):
            grad = dot(dq[...], w_q_v[columns(l), :], 1, 1) * dgain[:, columns(l)]
            gn[l] = grad
            return total + jnp.sum(
                grad * tok_v[:, columns(l)].astype(F32), axis=-1, keepdims=True
            )

        total = lax.fori_loop(0, lanes, backward, jnp.zeros((high, 1), F32))
        scale = tscale[...]
        tilt = total * scale * scale / (lanes * cols)

        def finish(l):
            grad = scale * (gn[l] - tok_v[:, columns(l)].astype(F32) * tilt)
            outs[l // 2, lax.rem(l, 2), 1] = grad.astype(BF16)

        loop(lanes, finish)

    def out_pair(k, h):
        return rcopy(
            outs.at[k, 1 - c, h], osib.at[k, h], o_send.at[h, k], o_recv.at[h, k], mp_1=1 - c
        )

    def out_piece(k, h, to, dst, sem):
        return rcopy(ocomb.at[k, h], dst, o_send.at[h, sem], o_recv.at[h, sem], mp_0=to)

    def out_relay(h):
        return out_piece(opp, h, toward[h], orelay.at[h], nx)

    def out_plain(h):
        to = toward[1 - h]
        return out_piece(to, h, to, fin.at[1 - h, h], nx + 1)

    def out_final(h):
        to = toward[h]
        return out_piece(to, h, to, fin.at[h, h], nx + 2)

    def out_open(h):
        for k in (opp, left, right, x):
            out_pair(k, h).start()

    def by_stretch(f):
        loop(high // STRETCH, lambda i: f(pl.ds(pl.multiple_of(i * STRETCH, STRETCH), STRETCH)))

    def out_reduce_pair(h):
        def add(k):
            out_pair(k, h).wait_recv()

            def go(at):
                ocomb[k, h, at, :] = (
                    outs[k, c, h, at, :].astype(F32) + osib[k, h, at, :].astype(F32)
                ).astype(BF16)

            by_stretch(go)

        add(opp)
        out_relay(h).start()
        add(toward[1 - h])
        out_plain(h).start()
        add(toward[h])
        add(x)

    def out_reduce_ends(h):
        out_relay(h).wait_recv()

        def go(at):
            ocomb[toward[h], h, at, :] = (
                ocomb[toward[h], h, at, :].astype(F32) + orelay[h, at, :].astype(F32)
            ).astype(BF16)

        by_stretch(go)
        out_final(h).start()

    def out_close(h, target):
        out_plain(h).wait_recv()
        out_final(h).wait_recv()

        def go(at):
            total = ocomb[x, h, at, :].astype(F32) + fin[0, h, at, :].astype(F32)
            target[at, :] = (total + fin[1, h, at, :].astype(F32)).astype(target.dtype)

        by_stretch(go)

    m = len(aft)
    for i in range(m):
        terms_of(i)
        each(pair_start, i)
    loop(n_seq, find_back, 2)
    out_terms()
    out_open(0)
    each(reduce_pair, 0)
    each(reduce_pair, 1)
    grad_terms()
    out_open(1)
    each(reduce_ends, 0)
    for i in range(2, m):
        each(reduce_pair, i)
    out_reduce_pair(0)
    each(reduce_ends, 1)
    each(give_back, 0)
    for i in range(2, m):
        each(reduce_ends, i)
    out_reduce_pair(1)
    each(give_back, 1)
    out_reduce_ends(0)
    for i in range(2, m):
        each(give_back, i)
    out_reduce_ends(1)

    def collect(n, i):
        returns[n][i][1]()
        if n == 2:
            shared(i).start()
        else:
            shared(i).wait_recv()

    def tally(i):
        l0, w = aft[i]
        for u in range(2):
            def add(d, sums):
                named = name_s[d]
                slot = got_back[i][d, u].astype(F32)
                return tuple(
                    total + jnp.where(named == r, slot, 0.0) for r, total in enumerate(sums)
                )

            sums = lax.fori_loop(
                0, n_seq, add, tuple(jnp.zeros((UNIT, w), F32) for _ in range(rows_dev)), unroll=2
            )
            for r in range(rows_dev):
                acc[r, u, :, l0:l0 + w] = sums[r]
        part = acc[:, :, :, l0:l0 + w].reshape(units, w).astype(BF16)
        out = dot(part, w_out_v[:, l0:l0 + w], 1, 1)
        grad_hid[...] = out if i == 0 else grad_hid[...] + out

    for i in range(len(aft)):
        each(collect, i)
        tally(i)
        if i == m - 2:
            out_close(0, cca)
            out_close(1, gtok)

    values = win_v[...].astype(F32).reshape(units, e)
    scaling = rms_scaling(values)
    unit = values * scaling
    g = dot((grad_hid[...] * slope[...]).astype(BF16), w_in_v[...], 1, 1) * egain[...].reshape(1, e)
    grad_enc = acc[...].reshape(units, e)
    out = grad_enc + scaling * (g - unit * jnp.mean(g * unit, axis=-1, keepdims=True))
    out = out.reshape(rows_dev, 2 * UNIT, e)
    keep = gdb.shape[0]
    for n in range(2):
        @pl.when(c == n)
        def _(n=n):
            at = (2 * UNIT - keep) * n
            gdb[...] = jnp.swapaxes(out[:, at:at + keep, :], 0, 1)

    def drain(n):
        for i in range(len(fore)):
            ask[n][i][2]()
            for copy in ring_copies(n, i):
                copy.wait_send()
        for i in range(len(aft)):
            returns[n][i][2]()
            for k in range(nx):
                pair_copy(n, i, k, 3 - n).wait_send()
            for h in range(2):
                for copy in (relay_of(n, i, h), plain_of(n, i, h), final_of(n, i, h)):
                    copy.wait_send()
            if n == 2:
                shared(i).wait_send()

    each(drain)
    for h in range(2):
        for copy in [out_pair(k, h) for k in range(nx)] + [out_relay(h), out_plain(h), out_final(h)]:
            copy.wait_send()


def step(dims, *args):
    n_seq, nx, nb, rows_dev, e, fore, aft = dims
    shards, rows_in, db, egain, w_in, w_out, tok, gout, dgain, w_q, w_p, w_k, w_v = args
    slot = (2, UNIT, e)
    high, width = tok.shape[0], w_q.shape[1]
    lanes = 2 * nx
    cols = tok.shape[1] // lanes
    half = nb // 2
    units = rows_dev * 2 * UNIT
    rows = nb * 3 * nx * UNIT
    nf, na = len(fore), len(aft)
    dma = pltpu.SemaphoreType.DMA
    return pl.pallas_call(
        functools.partial(step_kernel, dims),
        out_shape=(
            jax.ShapeDtypeStruct((high, cols), BF16),
            jax.ShapeDtypeStruct((high, cols), F32),
            jax.ShapeDtypeStruct((3 * UNIT // 2, rows_dev, e), F32),
        ),
        in_specs=[SM, SM, HB, VM, HB, HB, HB, HB, VM, HB, HB, HB, HB],
        out_specs=(VM, VM, VM),
        scratch_shapes=[
            pltpu.VMEM((rows_dev, *slot), BF16),
            *[pltpu.VMEM(a.shape, BF16) for a in (w_in, w_out, tok, gout, w_q, w_p, w_k, w_v)],
            pltpu.VMEM((rows_dev, *slot), BF16),
            pltpu.VMEM((units, w_in.shape[1]), F32),
            pltpu.VMEM((n_seq, *slot), BF16),
            [pltpu.VMEM((n_seq, 2, UNIT, w), BF16) for _, w in fore],
            pltpu.VMEM((nb, 3 * nx, UNIT, e), BF16),
            pltpu.VMEM((high, width), BF16),
            pltpu.VMEM((high, width), BF16),
            pltpu.VMEM((high, 1), F32),
            pltpu.VMEM((2, rows, width), F32),
            pltpu.VMEM((high, width), BF16),
            pltpu.VMEM((high, width), BF16),
            pltpu.VMEM((2, rows, width), BF16),
            pltpu.VMEM((nb, 3 * nx, UNIT, e), BF16),
            pltpu.VMEM((nx, nb, *slot), BF16),
            pltpu.VMEM((2, half, *slot), BF16),
            pltpu.VMEM((2, nb, *slot), BF16),
            pltpu.VMEM((nx, nb, *slot), BF16),
            pltpu.VMEM((nb, *slot), BF16),
            [pltpu.VMEM((n_seq, 2, UNIT, w), BF16) for _, w in aft],
            [pltpu.VMEM((n_seq, 2, UNIT, w), BF16) for _, w in aft],
            pltpu.VMEM((rows_dev, *slot), F32),
            pltpu.VMEM((units, w_in.shape[1]), F32),
            pltpu.VMEM((lanes, high, cols), F32),
            pltpu.VMEM((nx, 2, 2, high, cols), BF16),
            pltpu.VMEM((nx, 2, high, cols), BF16),
            pltpu.VMEM((2, high, cols), BF16),
            pltpu.VMEM((nx, 2, high, cols), BF16),
            pltpu.VMEM((2, 2, high, cols), BF16),
            pltpu.SMEM((n_seq,), jnp.int32),
            pltpu.SMEM((n_seq,), jnp.int32),
            pltpu.SMEM((n_seq,), jnp.int32),
            dma((9,)),
            dma((nf,)),
            dma((nf,)),
            dma((nf, 11)),
            dma((nf, 11)),
            dma((na, nx + 6)),
            dma((na, nx + 6)),
            dma((2, nx + 3)),
            dma((2, nx + 3)),
            dma((na,)),
            dma((na,)),
            dma((na,)),
            dma((na,)),
        ],
        compiler_params=pltpu.CompilerParams(
            collective_id=0, has_side_effects=True, vmem_limit_bytes=BIG
        ),
        name="step",
    )(*[pltpu.with_memory_space_constraint(a, pltpu.HBM) for a in args])


def body(
    n_seq, nx,
    tokens, database, nb_shard, nb_row, dec_gain, enc_gain,
    w_in, w_out, w_query, w_key, w_value, w_proj, grad_out,
):
    rows_dev, length, e = database.shape
    nb = tokens.shape[0] // STRETCH * K
    dims = (n_seq, nx, nb, rows_dev, e, cuts(e, FORE), cuts(e, AFT))
    cca, gtok, gdb = step(
        dims, nb_shard.T, nb_row.T, database.reshape(rows_dev, length // UNIT, UNIT, e), enc_gain,
        w_in, w_out, tokens, grad_out, dec_gain.reshape(1, -1), w_query, w_proj, w_key, w_value,
    )
    return cca, gtok, jnp.swapaxes(gdb, 0, 1)


def solution(mesh):
    n_seq = mesh.shape["seq"]
    nx = mesh.shape["mp"] // 2
    split = Mesh(mesh.devices.reshape(n_seq, nx, 2), ("seq", "mp_0", "mp_1"))
    placed = (
        P("seq", None),
        P("seq", None, None),
        P(),
        P(),
        P(),
        P(),
        P(),
        P(),
        P(None, MP),
        P(None, MP),
        P(None, MP),
        P(MP, None),
        P("seq", None),
    )
    return jax.shard_map(
        functools.partial(body, n_seq, nx),
        mesh=split,
        in_specs=placed,
        out_specs=(P("seq", MP), P("seq", MP), P("seq", MP, None)),
        check_vma=False,
    )
```
